32 devices in a mesh: chan: 8 (over z, y), bins: 4 (over x, core).
Axes of the slice: x: 2, y: 2, z: 4, core: 2. Of those that a mesh axis runs over, the one named last changes fastest.
Arguments:
- effects: bfloat16 [64, 8192, 256], P('chan', 'bins'), may hold values from -0.19921875 to 0.19921875
- nominal: float32 [64, 8192], P('chan', 'bins'), may hold values from 0.2 to 5
- observed: int32 [64, 8192], P('chan', 'bins'), may hold values from 0 to 7
- mc_variance: float32 [64, 8192], P('chan', 'bins'), may hold values from 0.002 to 0.5
- theta: float32 [8192], replicated, may hold values from -4 to 4
- nuisance_index: int32 [64, 256], replicated, may hold values from 0 to 8191, as said below
- bin_counts: int32 [64], P('chan'), may hold values from 1 to 8192, 262144 in all
- tile_owner: int32 [256], replicated, may hold values from 0 to 255, each once
Outputs:
- hessian_tiles: float32 [256, 512, 512], P(('chan', 'bins'))
- gradient: float32 [8192], P(('chan', 'bins'))
The draws below stay inside these ranges and needn't reach their ends.
Inputs may be any that keep to these rules, and one draw needn't show every extreme that they name: `nuisance_index`: each channel's list is 2 runs of 128 consecutive nuisances, each run starting at a multiple of 128, the runs distinct and in increasing order. Bins at positions bin_counts[c] and beyond of channel c carry no data. `tile_owner`: every tile number appears exactly once.
All inputs are finite; a program needn't handle non-finite values. No bound on the sum of `bin_counts` on one device may be relied on, other than what follows from the above.
Results may differ from the reference program's by a relative error of at most 0.0029.
Values sent between devices are 32-bit elements; how exact they have to be, the bound alone decides.
A program may use at most 128 MiB of HBM per device.

```python
import math
import jax
import jax.numpy as jnp
import numpy as np
from jax import lax

NU = 8192
K = 256
GW = 128
TILE = 512
CH = 64
BC = 8192
NTS = 16
NT = 256


def draw_nuisance_index(key, part):
    group_count = NU // GW
    group_parts = K // GW
    channel_keys = jax.random.split(jax.random.fold_in(key, 17), CH)

    def one_channel(channel_key):
        shuffled = jax.random.permutation(channel_key, group_count)
        picked = jnp.sort(shuffled[:group_parts])
        return (picked[:, None] * GW + jnp.arange(GW)[None, :]).reshape(-1)
    return jax.vmap(one_channel)(channel_keys).astype(jnp.int32)


def with_ends(values, rng, least, top_value):
    dims = values.shape
    place = [jax.random.randint(jax.random.fold_in(rng, axis), (), 0, dims[axis]) for axis in range(len(dims))]
    values = values.at[tuple(place)].set(least)
    longest = dims.index(max(dims))
    place[longest] = (place[longest] + 1) % dims[longest]
    return values.at[tuple(place)].set(top_value)


def levels(stream_key, extent, shards, least, largest):
    factor_of = 1.0
    for position, shards_of in shards:
        steps = jax.random.uniform(jax.random.fold_in(jax.random.fold_in(stream_key, 6), position), (shards_of,), jnp.float32, least / len(shards), largest / len(shards))
        factor_of = factor_of * jnp.repeat(jnp.exp(steps), extent[position] // shards_of).reshape((-1,) + (1,) * (len(extent) - 1 - position))
    return factor_of


def split_up(amount, total, most, slope):
    loads = [(1 << 20) // math.isqrt(grade ** slope) + 1 for grade in range(2, amount + 1)]
    surplus, given = total - most - (amount - 1), [1] * (amount - 1)
    while surplus > 0:
        candidates = [i for i in range(amount - 1) if given[i] < most]
        whole, remaining = sum([loads[i] for i in candidates]), surplus
        for i in candidates:
            extra = min(most - given[i], max(1, remaining * loads[i] // whole), surplus)
            given[i] = given[i] + extra
            surplus = surplus - extra
    return np.array([most] + given)


def ragged_sizes(rng, number_of, total, limit, lean):
    if number_of == 2:
        one = jax.random.randint(rng, (), max(1, total - limit), min(limit, total - 1) + 1)
        return jnp.stack([one, total - one])
    tallies = jnp.asarray(split_up(number_of, total, limit, lean), jnp.int32)
    pairs = (number_of - 1) // 2
    giver, receiver = tallies[1:1 + 2 * pairs:2], tallies[2:2 + 2 * pairs:2]
    margin = jnp.minimum(giver - 1, limit - receiver)
    moved = jax.random.randint(jax.random.fold_in(rng, 1), (pairs,), 0, 1 << 20) % (margin + 1)
    tallies = tallies.at[1:1 + 2 * pairs:2].set(giver - moved).at[2:2 + 2 * pairs:2].set(receiver + moved)
    return tallies[jax.random.permutation(jax.random.fold_in(rng, 2), number_of)]


def gaussian(own_key, extent, spread, most, cuts=(), kind=jnp.bfloat16):
    level = levels(own_key, extent, cuts, -0.22, 0.18) if cuts else 1.0
    result = jax.random.normal(own_key, extent, jnp.float32) * spread * level
    return jnp.minimum(jnp.maximum(result, -most), most).astype(kind)


def setup_inputs(seed: int = 0) -> dict:
    arg_keys = jax.random.split(jax.random.key(seed), 9)
    return {
        "effects": gaussian(arg_keys[0], (CH, BC, K), 0.04, 0.19921875, ((0, 8), (1, 4))),
        "nominal": jnp.clip(jnp.exp(math.log(5.0) - 3.218876 * jax.random.uniform(arg_keys[1], (CH, BC), jnp.float32) ** levels(arg_keys[1], (CH, BC), ((0, 8), (1, 4)), -0.2, 0.2)), 0.2, 5.0),
        "observed": with_ends(jax.random.randint(arg_keys[2], (CH, BC), 0, 8), jax.random.fold_in(arg_keys[2], 1), 0, 7).astype(jnp.int32),
        "mc_variance": jnp.clip(jnp.exp(math.log(0.5) - 5.521461 * jax.random.uniform(arg_keys[3], (CH, BC), jnp.float32) ** levels(arg_keys[3], (CH, BC), ((0, 8), (1, 4)), -0.2, 0.2)), 0.002, 0.5),
        "theta": gaussian(arg_keys[4], (NU,), 1.0, 4.0, (), jnp.float32),
        "nuisance_index": draw_nuisance_index(jax.random.fold_in(arg_keys[8], 71), 0),
        "bin_counts": ragged_sizes(arg_keys[6], CH, CH * BC // 2, BC, 2).astype(jnp.int32),
        "tile_owner": jax.random.permutation(arg_keys[7], NT).astype(jnp.int32),
    }


def reference(effects, nominal, observed, mc_variance, theta, nuisance_index, bin_counts, tile_owner):
    positions = jnp.arange(BC, dtype=jnp.int32)

    def channel_step(carry, inputs):
        hessian, gradient = carry
        matrix, nominal_row, observed_row, variance_row, indices, used = inputs
        chosen = theta[indices].astype(jnp.bfloat16)
        exponent = jnp.dot(matrix, chosen, preferred_element_type=jnp.float32)
        expected = nominal_row * jnp.exp(exponent)
        denominator = 1.0 + expected * variance_row
        live = positions < used
        residual = jnp.where(live, (expected - observed_row) / denominator, 0.0)
        weight = jnp.where(live, expected / denominator, 0.0)
        scaled = (jnp.sqrt(weight)[:, None] * matrix).astype(jnp.bfloat16)
        block = jnp.dot(scaled.T, scaled, preferred_element_type=jnp.float32)
        gradient_part = jnp.dot(residual.astype(jnp.bfloat16), matrix, preferred_element_type=jnp.float32)
        hessian = hessian.at[indices[:, None], indices[None, :]].add(block)
        gradient = gradient.at[indices].add(gradient_part)
        return ((hessian, gradient), None)
    initial = (jnp.zeros((NU, NU), jnp.float32), jnp.zeros((NU,), jnp.float32))
    totals, ignored = lax.scan(channel_step, initial, (effects, nominal, observed, mc_variance, nuisance_index, bin_counts))
    hessian = totals[0] + jnp.eye(NU, dtype=jnp.float32)
    tiles = hessian.reshape(NTS, TILE, NTS, TILE).transpose(0, 2, 1, 3).reshape(NT, TILE, TILE)
    return (tiles[tile_owner], totals[1] + theta)
```

```python
import functools

import jax
import jax.numpy as jnp
from jax import lax
from jax.experimental import pallas as pl
from jax.experimental.pallas import tpu as pltpu
from jax.sharding import PartitionSpec as P

GW = 128
TILE = 512
EXTRA = 8


def channel_payload(eff, chosen, nominal, observed, variance, live):
    eff_t = eff.T
    exponent = jnp.dot(chosen, eff_t, preferred_element_type=jnp.float32)[0:8]
    expected = nominal * jnp.exp(exponent)
    denominator = 1.0 + expected * variance
    residual = jnp.where(live, (expected - observed) / denominator, 0.0)
    weight = jnp.where(live, expected / denominator, 0.0)
    weighted = (eff_t.astype(jnp.float32) * weight[0:1]).astype(jnp.bfloat16)
    residual_rows = jnp.concatenate([residual, residual], axis=0).astype(jnp.bfloat16)
    left = jnp.concatenate([weighted, residual_rows], axis=0)
    full = jnp.dot(left, eff, preferred_element_type=jnp.float32)
    first, off, second = full[:GW, :GW], full[:GW, GW:], full[GW : 2 * GW, GW:]
    row = lax.broadcasted_iota(jnp.int32, (GW, GW), 0)
    col = lax.broadcasted_iota(jnp.int32, (GW, GW), 1)
    packed = jnp.where(row <= col, first, second)
    second_diag = jnp.sum(jnp.where(row == col, second, 0.0), axis=0, keepdims=True)
    grad0 = full[2 * GW : 2 * GW + 8, :GW]
    grad1 = full[2 * GW : 2 * GW + 8, GW:]
    which = lax.broadcasted_iota(jnp.int32, (EXTRA, GW), 0)
    extra = jnp.where(
        which == 0, grad0, jnp.where(which == 1, grad1, jnp.broadcast_to(second_diag, (EXTRA, GW)))
    )
    return packed, off, extra


def curvature_kernel(groups_ref, counts_ref, eff_ref, nom_ref, obs_ref, var_ref, theta_ref, out_ref):
    chan = lax.axis_index("chan")
    bins = lax.axis_index("bins")
    c = pl.program_id(0)
    size = eff_ref.shape[1]
    base = chan * pl.num_programs(0) + c
    g0, g1 = groups_ref[base, 0], groups_ref[base, 1]
    chosen = jnp.concatenate([theta_ref[g0], theta_ref[g1]], axis=1).astype(jnp.bfloat16)
    chosen = jnp.broadcast_to(chosen, (16, 2 * GW))
    line = pl.ds(c, 1)
    nominal, observed, variance = nom_ref[line], obs_ref[line].astype(jnp.float32), var_ref[line]
    position = bins * size + lax.broadcasted_iota(jnp.int32, (8, size), 1)
    packed, off, extra = channel_payload(
        eff_ref[0], chosen, nominal, observed, variance, position < counts_ref[c]
    )
    out_ref[0, :GW] = packed
    out_ref[0, GW : 2 * GW] = off
    out_ref[0, 2 * GW :] = extra


def curvature(effects, nominal, observed, variance, theta, groups, counts):
    chans, size, width = effects.shape
    rows = 2 * GW + EXTRA
    whole = lambda *shape: pl.BlockSpec(shape, lambda c, *_: (0,) * len(shape))
    return pl.pallas_call(
        curvature_kernel,
        grid_spec=pltpu.PrefetchScalarGridSpec(
            num_scalar_prefetch=2,
            grid=(chans,),
            in_specs=[
                pl.BlockSpec((1, size, width), lambda c, *_: (c, 0, 0)),
                whole(chans, size),
                whole(chans, size),
                whole(chans, size),
                whole(theta.shape[0] // GW, 1, GW),
            ],
            out_specs=pl.BlockSpec((1, rows, GW), lambda c, *_: (c, 0, 0)),
        ),
        out_shape=jax.ShapeDtypeStruct((chans, rows, GW), jnp.float32),
        compiler_params=pltpu.CompilerParams(vmem_limit_bytes=58 * 2**20),
        name="curvature",
    )(
        groups,
        counts,
        effects,
        nominal,
        observed,
        variance,
        theta.reshape(-1, 1, GW),
    )


def place_kernel(
    groups_ref, owner_ref, payload_ref, theta_ref, tiles_ref, grad_ref,
    lookup, entries, counts,
):
    step = pl.program_id(0)
    slots = counts.shape[0] - 1
    device = lax.axis_index("chan") * lax.axis_size("bins") + lax.axis_index("bins")
    chans = payload_ref.shape[0]
    per_tile = TILE // GW
    total_groups = theta_ref.shape[0]
    side = total_groups // per_tile
    shift = per_tile.bit_length() - 1
    room = 4 * chans
    start = device * slots

    @pl.when(step == 0)
    def _():
        def clear(i, _):
            for j in range(16):
                lookup[i * 16 + j] = slots
            return 0

        lax.fori_loop(0, side * side // 16, clear, 0)
        counts[slots] = 0
        for s in range(slots):
            counts[s] = 0
            lookup[owner_ref[start + s]] = s

        def visit(pair, _):
            for c in (pair * 2, pair * 2 + 1):
                a, b = groups_ref[c, 0], groups_ref[c, 1]
                ta, tb = a >> shift, b >> shift
                ra, rb = a & (per_tile - 1), b & (per_tile - 1)
                cases = ((ta, ta, ra, ra), (tb, tb, rb, rb), (ta, tb, ra, rb), (tb, ta, rb, ra))
                for kind, (tr, tc, rr, rc) in enumerate(cases):
                    slot = lookup[tr * side + tc]
                    n = counts[slot]
                    entries[slot * room + n] = ((((c << shift) + rr) << shift) + rc) * 4 + kind
                    counts[slot] = n + 1
            return 0

        lax.fori_loop(0, chans // 2, visit, 0)

    tile = owner_ref[start + step]

    tiles_ref[...] = jnp.zeros_like(tiles_ref)
    eye = (
        lax.broadcasted_iota(jnp.int32, (GW, GW), 0) == lax.broadcasted_iota(jnp.int32, (GW, GW), 1)
    ).astype(jnp.float32)

    @pl.when(tile // side == tile % side)
    def _():
        for r in range(per_tile):
            tiles_ref[0, r * GW : (r + 1) * GW, r * GW : (r + 1) * GW] = eye

    row = lax.broadcasted_iota(jnp.int32, (GW, GW), 0)
    col = lax.broadcasted_iota(jnp.int32, (GW, GW), 1)

    def accumulate(i, _):
        code = entries[step * room + i]
        kind = code & 3
        rc = (code >> 2) & (per_tile - 1)
        rr = (code >> (2 + shift)) & (per_tile - 1)
        c = code >> (2 + 2 * shift)
        at = (
            0,
            pl.ds(pl.multiple_of(rr * GW, GW), GW),
            pl.ds(pl.multiple_of(rc * GW, GW), GW),
        )

        @pl.when(kind == 0)
        def _():
            upper = jnp.where(row <= col, payload_ref[c, :GW], 0.0)
            tiles_ref[at] += upper + jnp.where(row > col, upper.T, 0.0)

        @pl.when(kind == 1)
        def _():
            lower = jnp.where(row > col, payload_ref[c, :GW], 0.0)
            diag = jnp.where(row == col, payload_ref[c, 2 * GW + 2 : 2 * GW + 3], 0.0)
            tiles_ref[at] += lower + lower.T + diag

        @pl.when(kind == 2)
        def _():
            tiles_ref[at] += payload_ref[c, GW : 2 * GW]

        @pl.when(kind == 3)
        def _():
            tiles_ref[at] += payload_ref[c, GW : 2 * GW].T

        return 0

    lax.fori_loop(0, counts[step], accumulate, 0)

    @pl.when(step == slots - 1)
    def _():
        mine = grad_ref.shape[0]
        first = device * total_groups // (lax.axis_size("chan") * lax.axis_size("bins"))
        for m in range(mine):
            grad_ref[m] = theta_ref[first + m]

        def add(c, _):
            for r in range(2):
                m = groups_ref[c, r] - first

                @pl.when(jnp.logical_and(m >= 0, m < mine))
                def _(m=m, r=r):
                    grad_ref[m] += payload_ref[c, 2 * GW + r : 2 * GW + r + 1]

            return 0

        lax.fori_loop(0, chans, add, 0)


def place(payload, theta, groups, tile_owner, slots, mine):
    chans, rows = payload.shape[:2]
    return pl.pallas_call(
        place_kernel,
        grid_spec=pltpu.PrefetchScalarGridSpec(
            num_scalar_prefetch=2,
            grid=(slots,),
            in_specs=[
                pl.BlockSpec(memory_space=pltpu.VMEM),
                pl.BlockSpec((theta.shape[0] // GW, 1, GW), lambda s, *_: (0, 0, 0)),
            ],
            out_specs=[
                pl.BlockSpec((1, TILE, TILE), lambda s, *_: (s, 0, 0)),
                pl.BlockSpec((mine, 1, GW), lambda s, *_: (0, 0, 0)),
            ],
            scratch_shapes=[
                pltpu.SMEM((tile_owner.shape[0],), jnp.int32),
                pltpu.SMEM(((slots + 1) * chans * 4,), jnp.int32),
                pltpu.SMEM((slots + 1,), jnp.int32),
            ],
        ),
        out_shape=[
            jax.ShapeDtypeStruct((slots, TILE, TILE), jnp.float32),
            jax.ShapeDtypeStruct((mine, 1, GW), jnp.float32),
        ],
        compiler_params=pltpu.CompilerParams(
            vmem_limit_bytes=4 * chans * (rows + EXTRA) * GW + 8 * 2**20
        ),
        name="place",
    )(groups, tile_owner, payload, theta.reshape(-1, 1, GW))


COLORS = ((0, 104, "zxy"), (104, 96, "zyx"), (200, 64, "xyz"))
DEEP = 4
LINKS = 5


def exponent_rows(eff, chosen, nominal, observed, variance, live, left_ref):
    eff_t = eff.T
    exponent = jnp.dot(chosen, eff_t, preferred_element_type=jnp.float32)[0:8]
    expected = nominal * jnp.exp(exponent)
    denominator = 1.0 + expected * variance
    residual = jnp.where(live, (expected - observed) / denominator, 0.0)
    weight = jnp.where(live, expected / denominator, 0.0)
    left_ref[: 2 * GW] = (eff_t.astype(jnp.float32) * weight[0:1]).astype(jnp.bfloat16)
    left_ref[2 * GW :] = jnp.concatenate([residual, residual], axis=0).astype(jnp.bfloat16)


def block_rows(left, eff):
    full = jnp.dot(left, eff, preferred_element_type=jnp.float32)
    first, off, second = full[:GW, :GW], full[:GW, GW:], full[GW : 2 * GW, GW:]
    row = lax.broadcasted_iota(jnp.int32, (GW, GW), 0)
    col = lax.broadcasted_iota(jnp.int32, (GW, GW), 1)
    packed = jnp.where(row <= col, first, second)
    second_diag = jnp.sum(jnp.where(row == col, second, 0.0), axis=0, keepdims=True)
    grad0 = full[2 * GW : 2 * GW + 8, :GW]
    grad1 = full[2 * GW : 2 * GW + 8, GW:]
    which = lax.broadcasted_iota(jnp.int32, (EXTRA, GW), 0)
    extra = jnp.where(
        which == 0, grad0, jnp.where(which == 1, grad1, jnp.broadcast_to(second_diag, (EXTRA, GW)))
    )
    return packed, off, extra


def make_plan(index_ref, mine, total_groups, plan_ref):
    per_tile = TILE // GW
    shift = per_tile.bit_length() - 1
    side = total_groups // per_tile
    chans = index_ref.shape[0]
    slots = len(mine)
    count = 4 * chans
    gshift = GW.bit_length() - 1
    a, b = index_ref[:, :GW] >> gshift, index_ref[:, GW:] >> gshift
    ta, tb = a >> shift, b >> shift
    ra, rb = a & (per_tile - 1), b & (per_tile - 1)
    c = lax.broadcasted_iota(jnp.int32, (chans, GW), 0)
    keys, codes, places = [], [], []
    cases = ((ta, ta, ra, ra), (tb, tb, rb, rb), (ta, tb, ra, rb), (tb, ta, rb, ra))
    for kind, (tr, tc, rr, rc) in enumerate(cases):
        tile = tr * side + tc
        slot = jnp.full((chans, GW), slots, jnp.int32)
        for s in range(slots):
            slot = jnp.where(tile == mine[s], s, slot)
        places.append(slot)
        keys.append(slot * count + kind * chans + c)
        codes.append(((((c << shift) + rr) << shift) + rc) * 4 + kind)
    key = jnp.concatenate(keys, axis=0)
    code = jnp.concatenate(codes, axis=0).astype(jnp.float32)
    place_col = jnp.concatenate(places, axis=0)
    lane = lax.broadcasted_iota(jnp.int32, (count, GW), 1)
    key_rows = key.T
    rank = jnp.zeros((count, 1), jnp.float32)
    for j in range(0, count, GW):
        less = jnp.where(key_rows[0:1, j : j + GW] < key, 1.0, 0.0)
        rank += jnp.sum(less, axis=1, keepdims=True)
    rank = jnp.broadcast_to(rank, (count, GW)).astype(jnp.int32)
    for j in range(0, count, GW):
        picked = jnp.sum(jnp.where(rank == lane + j, code, 0.0), axis=0, keepdims=True)
        plan_ref[0:1, j : j + GW] = picked.astype(jnp.int32)
    starts = jnp.sum(jnp.where(place_col < lane, 1.0, 0.0), axis=0, keepdims=True)
    plan_ref[1:2, 0:GW] = starts.astype(jnp.int32)
    lane1 = lax.broadcasted_iota(jnp.int32, (1, GW), 1)
    diagonal = jnp.zeros((1, GW), jnp.int32)
    for s in range(slots):
        t = jnp.full((1, GW), mine[s], jnp.int32)
        on = (t >> (side.bit_length() - 1)) == (t & (side - 1))
        diagonal = jnp.where(jnp.logical_and(lane1 == s, on), 1, diagonal)
    plan_ref[2:3, 0:GW] = diagonal


def exchange_kernel(
    ydim, slots, index_hbm, counts_hbm, eff_hbm, nom_hbm, obs_hbm, var_hbm, theta_hbm, owner_hbm,
    out_ref, plan_ref,
    eff_held, parts_ref, swap, cross, total, left, nom_ref, obs_ref, var_ref, theta_ref, index_ref,
    local_index, counts_ref, owner_ref,
    eff_sem, small_sem, swap_recv, cross_recv, recv, drecv, send,
):
    chan, bins = lax.axis_index("chan"), lax.axis_index("bins")
    zdim = lax.axis_size("chan") // ydim
    nbins = lax.axis_size("bins")
    z, y = chan // ydim, chan % ydim
    x, core = bins // 2, bins % 2
    chans, size = eff_held.shape[:2]
    held = chans // nbins
    sent = {}
    colors = len(COLORS)

    def device(zz, yy, xx, kk):
        return {"chan": zz * ydim + yy, "bins": xx * 2 + kk}

    def run(cond, action):
        if cond is None:
            action()
        else:
            pl.when(cond)(action)

    def copy(src, dst, recv_sem, target, group, there=None):
        made = pltpu.make_async_remote_copy(
            src_ref=src,
            dst_ref=dst,
            send_sem=send.at[group],
            recv_sem=recv_sem,
            device_id=target,
            device_id_type=pl.DeviceIdType.MESH,
        )
        cond, places = (None, range(zdim)) if there is None else there
        counted = sent.setdefault(group, [0] * zdim)
        for place in places:
            counted[place] += 1
        run(cond, made.start)

    far, near = (1 - x) * 2, x * 2
    owners = (far + 1 - core, far + core, near + 1 - core, near + core)

    def load(q, h):
        at = q * held + h
        return pltpu.make_async_copy(eff_hbm.at[owners[q] * held + h], eff_held.at[at], eff_sem.at[at])

    mine_rows = pl.ds(pl.multiple_of(chan * chans, chans), chans)
    smalls = [
        (index_hbm.at[mine_rows], local_index),
        (counts_hbm, counts_ref),
        (theta_hbm, theta_ref),
        (nom_hbm, nom_ref),
        (var_hbm, var_ref),
        (obs_hbm, obs_ref),
        (owner_hbm, owner_ref),
        (index_hbm, index_ref),
    ]
    smalls = [pltpu.make_async_copy(a, b, small_sem.at[n]) for n, (a, b) in enumerate(smalls)]
    for made in smalls[:3]:
        made.start()
    load(0, 0).start()
    for made in smalls[3:6]:
        made.start()
    for h in range(held):
        for q in range(4):
            if (q, h) != (0, 0):
                load(q, h).start()
    for made in smalls[6:]:
        made.start()

    partner = device(z, y, x, 1 - core)
    beside = device(z, y, 1 - x, core)
    below_there, above_there = z > 0, z < zdim - 1

    barrier = pltpu.get_barrier_semaphore()
    for target, cond in (
        (partner, None),
        (beside, None),
        (device(z, 1 - y, x, core), None),
        (device(z - 1, y, x, core), below_there),
        (device(z + 1, y, x, core), above_there),
    ):
        run(cond, lambda target=target: pl.semaphore_signal(
            barrier, 1, device_id=target, device_id_type=pl.DeviceIdType.MESH
        ))
    for made in smalls[:6]:
        made.wait()

    def prepare(q, h):
        c = owners[q] * held + h
        g0 = local_index[c, 0] >> (GW.bit_length() - 1)
        g1 = local_index[c, GW] >> (GW.bit_length() - 1)
        chosen = jnp.concatenate([theta_ref[g0], theta_ref[g1]], axis=1).astype(jnp.bfloat16)
        chosen = jnp.broadcast_to(chosen, (16, 2 * GW))
        line = pl.ds(c, 1)
        position = bins * size + lax.broadcasted_iota(jnp.int32, (8, size), 1)
        exponent_rows(
            eff_held[q * held + h],
            chosen,
            nom_ref[line],
            obs_ref[line].astype(jnp.float32),
            var_ref[line],
            position < counts_ref[c],
            left.at[q % 2],
        )

    def multiply(q, h):
        packed, off, extra = block_rows(left[q % 2], eff_held[q * held + h])
        at = q * held + h
        parts_ref[at, :GW] = packed
        parts_ref[at, GW : 2 * GW] = off
        parts_ref[at, 2 * GW :] = extra

    steps = [(q, h) for h in range(held) for q in range(4)]

    def compute(n):
        if n == 0:
            load(*steps[0]).wait()
            prepare(*steps[0])
        if n + 1 < len(steps):
            load(*steps[n + 1]).wait()
            prepare(*steps[n + 1])
        multiply(*steps[n])

    def arrived(dst, sem):
        pltpu.make_async_remote_copy(
            src_ref=dst, dst_ref=dst, send_sem=send.at[0], recv_sem=sem,
            device_id=partner, device_id_type=pl.DeviceIdType.MESH,
        ).wait_recv()

    def to_partner(q, h):
        n = q // 2 * held + h
        copy(parts_ref.at[q * held + h], swap.at[n], swap_recv.at[n], partner, LINKS * colors)

    def send_across(h):
        arrived(swap.at[h], swap_recv.at[h])
        total[h] = parts_ref[held + h] + swap[h]
        for color, (first, count, _) in enumerate(COLORS):
            rows = pl.ds(first, count)
            copy(total.at[h, rows], cross.at[h, rows], cross_recv.at[h, color], beside, 2 * colors + color)

    own = (chan * nbins + bins) * held

    def finish(h, color):
        first, count, _ = COLORS[color]
        rows = pl.ds(first, count)
        arrived(cross.at[h, rows], cross_recv.at[h, color])
        out_ref[own + h, rows] = (
            parts_ref[3 * held + h, rows] + swap[held + h, rows]
        ) + cross[h, rows]

    def forward(h, color, dz, fx, fy):
        first, count, order = COLORS[color]
        sz, sx, sy = z + dz, (1 - x if fx else x), (1 - y if fy else y)
        chip = (sz * ydim + sy) * 2 + sx
        there = None if dz == 0 else (z >= -dz if dz < 0 else z < zdim - dz)
        places = [p for p in range(zdim) if 0 <= p + dz < zdim]
        at = ((sz * ydim + sy) * nbins + sx * 2 + core) * held + h
        piece = out_ref.at[at, pl.ds(first, count)]
        offset = {"z": dz, "x": fx, "y": fy}
        last = max([n for n, d in enumerate(order) if offset[d]], default=-1)
        sem = recv.at[h, color, chip]
        if last >= 0:
            run(there, lambda: arrived(piece, sem))

        def both(a, b):
            return b if a is None else (a if b is None else jnp.logical_and(a, b))

        here = (there, places)
        if zdim > 1:
            onward = order.index("z") > last
            if (onward or (last >= 0 and order[last] == "z" and dz < 0)) and dz >= 2 - zdim:
                up = (both(there, above_there), [p for p in places if p < zdim - 1])
                copy(piece, piece, sem, device(z + 1, y, x, core), color, up)
            if (onward or (last >= 0 and order[last] == "z" and dz > 0)) and dz <= zdim - 2:
                down = (both(there, below_there), [p for p in places if p > 0])
                copy(piece, piece, sem, device(z - 1, y, x, core), colors + color, down)
        if order.index("x") > last:
            copy(piece, piece, sem, beside, 2 * colors + color, here)
        if order.index("y") > last:
            copy(piece, piece, sem, device(z, 1 - y, x, core), 3 * colors + color, here)
        copy(piece, piece, drecv.at[color], partner, 4 * colors + color, here)

    compute(0)
    pl.semaphore_wait(barrier, 3 + jnp.minimum(z, 1) + jnp.minimum(zdim - 1 - z, 1))
    to_partner(0, 0)
    compute(1)
    send_across(0)
    compute(2)
    to_partner(2, 0)
    compute(3)
    compute(4)
    to_partner(0, 1)
    compute(5)
    send_across(1)
    arrived(swap.at[held], swap_recv.at[held])
    finish(0, 0)
    forward(0, 0, 0, 0, 0)
    compute(6)
    to_partner(2, 1)
    finish(0, 1)
    forward(0, 1, 0, 0, 0)
    compute(7)
    finish(0, 2)
    forward(0, 2, 0, 0, 0)
    arrived(swap.at[held + 1], swap_recv.at[held + 1])
    order = [e for e in ORDER if abs(e[2]) < zdim]
    for n, e in enumerate(order):
        if n == PLAN_AT:
            for made in smalls[6:]:
                made.wait()
            me = (chan * nbins + bins) * slots
            make_plan(
                index_ref, [owner_ref[me + s] for s in range(slots)], theta_ref.shape[0], plan_ref
            )
        h, color, dz, fx, fy = e
        if (dz, fx, fy) == (0, 0, 0):
            finish(h, color)
        forward(*e)

    chips = zdim * ydim * 2

    def waiting(n, count, group, color):
        part = out_ref.at[pl.ds(0, n), pl.ds(0, count)]
        return pltpu.make_async_remote_copy(
            src_ref=part, dst_ref=part, send_sem=send.at[group], recv_sem=drecv.at[color],
            device_id=partner, device_id_type=pl.DeviceIdType.MESH,
        )

    for color, (_, count, _) in enumerate(COLORS):
        waiting(held * chips, count, 0, color).wait_recv()
    for group, numbers in sent.items():
        count = COLORS[group % colors][1] if group < LINKS * colors else out_ref.shape[1]
        if len(set(numbers)) == 1:
            waiting(numbers[0], count, group, 0).wait_send()
            continue
        for place, number in enumerate(numbers):
            if number:
                pl.when(z == place)(waiting(number, count, group, 0).wait_send)


ORDER = (
    (1, 0, 0, 0, 0), (1, 1, 0, 0, 0), (1, 2, 0, 0, 0), (0, 0, -1, 0, 0), (0, 0, 1, 0, 0),
    (0, 1, -1, 0, 0), (1, 0, 1, 0, 0), (0, 1, 0, 0, 1), (1, 1, 1, 0, 0), (1, 0, -1, 0, 0),
    (1, 1, -1, 0, 0), (0, 2, -1, 0, 0), (0, 2, 0, 1, 0), (0, 0, 2, 0, 0), (0, 0, 0, 0, 1),
    (0, 0, 0, 1, 0), (1, 2, 0, 1, 0), (1, 0, -2, 0, 0), (0, 1, 1, 0, 0), (1, 2, 0, 0, 1),
    (0, 0, 1, 0, 1), (1, 0, 2, 0, 0), (0, 0, -2, 0, 0), (0, 2, 0, 0, 1), (1, 2, -1, 1, 0),
    (1, 0, 0, 1, 0), (0, 2, 1, 1, 0), (1, 1, 2, 0, 0), (1, 1, -2, 0, 0), (0, 2, 0, 1, 1),
    (1, 0, -3, 0, 0), (0, 1, -2, 0, 0), (0, 1, 2, 0, 0), (0, 2, 1, 0, 0), (0, 1, -1, 0, 1),
    (0, 0, -3, 0, 0), (1, 0, 3, 0, 0), (1, 0, 1, 0, 1), (1, 1, -3, 0, 0), (1, 0, -3, 1, 0),
    (0, 2, -1, 1, 0), (0, 2, -1, 0, 1), (0, 2, 2, 1, 0), (1, 0, -1, 1, 0), (1, 2, 1, 0, 0),
    (1, 1, 1, 0, 1), (1, 1, 3, 0, 0), (1, 2, -1, 0, 0), (0, 0, 2, 1, 0), (0, 1, 3, 0, 0),
    (1, 1, 0, 0, 1), (1, 2, 0, 1, 1), (1, 0, -2, 1, 0), (0, 1, -3, 0, 0), (1, 2, 1, 0, 1),
    (0, 0, 3, 0, 0), (1, 2, 1, 1, 0), (1, 1, 3, 1, 0), (0, 2, 1, 0, 1), (0, 0, -2, 0, 1),
    (1, 2, -1, 0, 1), (1, 2, -2, 1, 0), (1, 1, -3, 0, 1), (1, 0, -1, 0, 1), (0, 2, 3, 1, 0),
    (1, 0, 1, 1, 0), (0, 2, 2, 0, 0), (1, 0, -2, 0, 1), (1, 0, -3, 0, 1), (0, 1, 1, 0, 1),
    (0, 2, -2, 0, 0), (0, 2, -1, 1, 1), (1, 0, 3, 1, 0), (0, 2, 1, 1, 1), (1, 1, -3, 1, 0),
    (1, 1, 3, 0, 1), (0, 2, -2, 0, 1), (1, 0, 2, 1, 0), (1, 1, -2, 0, 1), (1, 0, 0, 1, 1),
    (0, 1, -2, 0, 1), (1, 0, 3, 0, 1), (1, 2, -1, 1, 1), (0, 0, -2, 1, 0), (0, 1, 1, 1, 0),
    (1, 1, 0, 1, 0), (0, 1, 3, 0, 1), (0, 0, -3, 1, 0), (1, 2, -2, 0, 0), (1, 2, 2, 0, 0),
    (0, 1, 2, 0, 1), (0, 0, -1, 0, 1), (0, 2, 3, 0, 0), (1, 2, 1, 1, 1), (1, 2, 2, 0, 1),
    (0, 0, 3, 1, 0), (1, 2, -2, 0, 1), (0, 1, -3, 1, 0), (0, 1, 2, 1, 0), (1, 1, 2, 0, 1),
    (1, 1, -1, 0, 1), (0, 0, 1, 1, 0), (1, 1, -3, 1, 1), (0, 2, -2, 1, 0), (0, 2, 2, 0, 1),
    (0, 0, 2, 0, 1), (0, 2, -2, 1, 1), (1, 1, 1, 1, 0), (1, 0, 2, 0, 1), (0, 1, 3, 1, 0),
    (0, 1, 3, 1, 1), (0, 0, -1, 1, 0), (0, 1, -3, 0, 1), (1, 2, 2, 1, 0), (0, 0, -3, 1, 1),
    (1, 2, -3, 1, 0), (0, 2, -3, 1, 0), (0, 1, 0, 1, 0), (0, 2, 3, 1, 1), (1, 2, 3, 0, 0),
    (1, 2, -2, 1, 1), (0, 2, -3, 0, 0), (0, 0, -2, 1, 1), (0, 0, -3, 0, 1), (0, 1, 0, 1, 1),
    (0, 0, 3, 1, 1), (0, 0, 3, 0, 1), (1, 0, 3, 1, 1), (1, 2, -3, 0, 0), (1, 0, -2, 1, 1),
    (0, 0, 0, 1, 1), (0, 1, -1, 1, 0), (0, 1, -1, 1, 1), (1, 1, 0, 1, 1), (1, 0, -1, 1, 1),
    (0, 1, -2, 1, 0), (1, 1, 1, 1, 1), (1, 2, 3, 0, 1), (0, 0, 2, 1, 1), (1, 0, 0, 0, 1),
    (0, 2, 2, 1, 1), (0, 2, 3, 0, 1), (1, 2, 2, 1, 1), (1, 0, 1, 1, 1), (1, 1, -2, 1, 1),
    (1, 1, 2, 1, 0), (0, 2, -3, 1, 1), (0, 0, 1, 1, 1), (0, 1, -2, 1, 1), (0, 1, 2, 1, 1),
    (1, 0, -3, 1, 1), (1, 2, -3, 0, 1), (0, 2, -3, 0, 1), (0, 1, 1, 1, 1), (1, 1, -2, 1, 0),
    (1, 1, -1, 1, 0), (1, 2, 3, 1, 0), (0, 0, -1, 1, 1), (1, 1, 2, 1, 1), (0, 1, -3, 1, 1),
    (1, 0, 2, 1, 1), (1, 1, 3, 1, 1), (1, 2, 3, 1, 1), (1, 1, -1, 1, 1), (1, 2, -3, 1, 1),
)
PLAN_AT = 40


def exchange(effects, nominal, observed, variance, theta, nuisance_index, counts, tile_owner):
    nbins, nchan = lax.axis_size("bins"), lax.axis_size("chan")
    chans, size, channel_width = effects.shape
    rows, width = 2 * GW + EXTRA, GW
    held = chans // nbins
    hbm = pl.BlockSpec(memory_space=pltpu.HBM)
    vmem = pl.BlockSpec(memory_space=pltpu.VMEM)
    chips = nchan * nbins // 2
    slots = tile_owner.shape[0] // (nchan * nbins)
    colors = len(COLORS)
    operands = (
        nuisance_index, counts, effects, nominal, observed, variance,
        theta.reshape(-1, 1, GW), tile_owner,
    )
    return pl.pallas_call(
        functools.partial(exchange_kernel, 2, slots),
        in_specs=[hbm] * len(operands),
        out_specs=[vmem, vmem],
        out_shape=[
            jax.ShapeDtypeStruct((nchan * chans, rows, width), jnp.float32),
            jax.ShapeDtypeStruct((8, 4 * nchan * chans), jnp.int32),
        ],
        scratch_shapes=[
            pltpu.VMEM((chans, size, channel_width), jnp.bfloat16),
            pltpu.VMEM((chans, rows, width), jnp.float32),
            pltpu.VMEM((2 * held, rows, width), jnp.float32),
            pltpu.VMEM((held, rows, width), jnp.float32),
            pltpu.VMEM((held, rows, width), jnp.float32),
            pltpu.VMEM((2, channel_width + 16, size), jnp.bfloat16),
            pltpu.VMEM(nominal.shape, nominal.dtype),
            pltpu.VMEM(observed.shape, observed.dtype),
            pltpu.VMEM(variance.shape, variance.dtype),
            pltpu.VMEM((theta.shape[0] // GW, 1, GW), theta.dtype),
            pltpu.VMEM(nuisance_index.shape, jnp.int32),
            pltpu.SMEM((chans, nuisance_index.shape[1]), jnp.int32),
            pltpu.SMEM(counts.shape, jnp.int32),
            pltpu.SMEM(tile_owner.shape, jnp.int32),
            pltpu.SemaphoreType.DMA((chans,)),
            pltpu.SemaphoreType.DMA((8,)),
            pltpu.SemaphoreType.DMA((2 * held,)),
            pltpu.SemaphoreType.DMA((held, colors)),
            pltpu.SemaphoreType.DMA((held, colors, chips)),
            pltpu.SemaphoreType.DMA((colors,)),
            pltpu.SemaphoreType.DMA((LINKS * colors + 1,)),
        ],
        compiler_params=pltpu.CompilerParams(
            collective_id=0, has_side_effects=True, vmem_limit_bytes=32 * 2**20
        ),
        name="exchange",
    )(*[pltpu.with_memory_space_constraint(a, pltpu.HBM) for a in operands])


def fill_kernel(plan_ref, payload_ref, index_ref, theta_ref, tiles_ref, grad_ref, held_tiles, sems):
    slots = held_tiles.shape[0]
    per_tile = TILE // GW
    shift = per_tile.bit_length() - 1
    row = lax.broadcasted_iota(jnp.int32, (GW, GW), 0)
    col = lax.broadcasted_iota(jnp.int32, (GW, GW), 1)
    eye = (row == col).astype(jnp.float32)

    def put(s):
        return pltpu.make_async_copy(held_tiles.at[s], tiles_ref.at[s], sems.at[s])

    def one_tile(s, _):
        held_tiles[s] = jnp.zeros((TILE, TILE), jnp.float32)

        @pl.when(plan_ref[2, s] == 1)
        def _():
            for r in range(per_tile):
                held_tiles[s, r * GW : (r + 1) * GW, r * GW : (r + 1) * GW] = eye

        def accumulate(i, _):
            code = plan_ref[0, i]
            kind = code & 3
            rc = (code >> 2) & (per_tile - 1)
            rr = (code >> (2 + shift)) & (per_tile - 1)
            c = code >> (2 + 2 * shift)
            at = (
                s,
                pl.ds(pl.multiple_of(rr * GW, GW), GW),
                pl.ds(pl.multiple_of(rc * GW, GW), GW),
            )

            @pl.when(kind == 0)
            def _():
                block = payload_ref[c, :GW]
                held_tiles[at] += jnp.where(row <= col, block, block.T)

            @pl.when(kind == 1)
            def _():
                block = payload_ref[c, :GW]
                diag = jnp.where(row == col, payload_ref[c, 2 * GW + 2 : 2 * GW + 3], block.T)
                held_tiles[at] += jnp.where(row > col, block, diag)

            @pl.when(kind == 2)
            def _():
                held_tiles[at] += payload_ref[c, GW : 2 * GW]

            @pl.when(kind == 3)
            def _():
                held_tiles[at] += payload_ref[c, GW : 2 * GW].T

            return 0

        lax.fori_loop(plan_ref[1, s], plan_ref[1, s + 1], accumulate, 0)
        put(s).start()
        return 0

    lax.fori_loop(0, slots, one_tile, 0)

    mine = grad_ref.shape[0]
    device = lax.axis_index("chan") * lax.axis_size("bins") + lax.axis_index("bins")
    total_groups = theta_ref.shape[0]
    first = device * total_groups // (lax.axis_size("chan") * lax.axis_size("bins"))
    gshift = GW.bit_length() - 1
    for m in range(mine):
        acc = theta_ref[first + m]
        for r in range(2):
            hit = (index_ref[:, r * GW : (r + 1) * GW] >> gshift) == first + m
            acc += jnp.sum(jnp.where(hit, payload_ref[:, 2 * GW + r], 0.0), axis=0, keepdims=True)
        grad_ref[m] = acc

    def drain(s, _):
        put(s).wait()
        return 0

    lax.fori_loop(0, slots, drain, 0)


def fill(payload, plan, theta, nuisance_index, slots, mine):
    chans, rows = payload.shape[:2]
    vmem = pl.BlockSpec(memory_space=pltpu.VMEM)
    return pl.pallas_call(
        fill_kernel,
        in_specs=[pl.BlockSpec(memory_space=pltpu.SMEM), vmem, vmem, vmem],
        out_specs=[pl.BlockSpec(memory_space=pltpu.HBM), vmem],
        out_shape=[
            jax.ShapeDtypeStruct((slots, TILE, TILE), jnp.float32),
            jax.ShapeDtypeStruct((mine, 1, GW), jnp.float32),
        ],
        scratch_shapes=[
            pltpu.VMEM((slots, TILE, TILE), jnp.float32),
            pltpu.SemaphoreType.DMA((slots,)),
        ],
        compiler_params=pltpu.CompilerParams(
            vmem_limit_bytes=4 * chans * (rows + EXTRA) * GW + 4 * slots * TILE * TILE + 4 * 2**20
        ),
        name="fill",
    )(plan, payload, nuisance_index, theta.reshape(-1, 1, GW))


def local(effects, nominal, observed, mc_variance, theta, nuisance_index, bin_counts, tile_owner):
    devices = lax.axis_size("chan") * lax.axis_size("bins")
    device = lax.axis_index("chan") * lax.axis_size("bins") + lax.axis_index("bins")
    total_nu = theta.shape[0]
    slice_len = total_nu // devices
    slots, mine = tile_owner.shape[0] // devices, max(1, slice_len // GW)
    chan_size, bins_size = lax.axis_size("chan"), lax.axis_size("bins")
    if bins_size == 4 and chan_size % 2 == 0 and chan_size // 2 <= DEEP and effects.shape[0] == 2 * bins_size and slice_len >= GW:
        payload, plan = exchange(
            effects, nominal, observed, mc_variance, theta, nuisance_index, bin_counts, tile_owner
        )
        tiles, grad = fill(payload, plan, theta, nuisance_index, slots, mine)
    else:
        groups = nuisance_index[:, ::GW] // GW
        arrays = (effects, nominal, observed, mc_variance, theta, groups, bin_counts)
        summed = lax.psum_scatter(curvature(*arrays), "bins", scatter_dimension=0, tiled=True)
        payload = lax.all_gather(summed, ("chan", "bins"), axis=0, tiled=True)
        tiles, grad = place(payload, theta, groups, tile_owner, slots, mine)
    gradient = grad.reshape(-1)
    if slice_len < GW:
        gradient = lax.dynamic_slice_in_dim(gradient, device * slice_len % GW, slice_len, 0)
    return (tiles, gradient)


def solution(mesh):
    return jax.shard_map(
        local,
        mesh=mesh,
        in_specs=(
            P("chan", "bins", None),
            P("chan", "bins"),
            P("chan", "bins"),
            P("chan", "bins"),
            P(),
            P(),
            P("chan"),
            P(),
        ),
        out_specs=(P(("chan", "bins"), None, None), P(("chan", "bins"))),
        check_vma=False,
    )
```

```python
import functools

import jax
import jax.numpy as jnp
from jax import lax
from jax.experimental import pallas as pl
from jax.experimental.pallas import tpu as pltpu
from jax.sharding import PartitionSpec as P

GW = 128
TILE = 512
EXTRA = 8


def channel_payload(eff, chosen, nominal, observed, variance, live):
    eff_t = eff.T
    exponent = jnp.dot(chosen, eff_t, preferred_element_type=jnp.float32)[0:8]
    expected = nominal * jnp.exp(exponent)
    denominator = 1.0 + expected * variance
    residual = jnp.where(live, (expected - observed) / denominator, 0.0)
    weight = jnp.where(live, expected / denominator, 0.0)
    weighted = (eff_t.astype(jnp.float32) * weight[0:1]).astype(jnp.bfloat16)
    residual_rows = jnp.concatenate([residual, residual], axis=0).astype(jnp.bfloat16)
    left = jnp.concatenate([weighted, residual_rows], axis=0)
    full = jnp.dot(left, eff, preferred_element_type=jnp.float32)
    first, off, second = full[:GW, :GW], full[:GW, GW:], full[GW : 2 * GW, GW:]
    row = lax.broadcasted_iota(jnp.int32, (GW, GW), 0)
    col = lax.broadcasted_iota(jnp.int32, (GW, GW), 1)
    packed = jnp.where(row <= col, first, second)
    second_diag = jnp.sum(jnp.where(row == col, second, 0.0), axis=0, keepdims=True)
    grad0 = full[2 * GW : 2 * GW + 8, :GW]
    grad1 = full[2 * GW : 2 * GW + 8, GW:]
    which = lax.broadcasted_iota(jnp.int32, (EXTRA, GW), 0)
    extra = jnp.where(
        which == 0, grad0, jnp.where(which == 1, grad1, jnp.broadcast_to(second_diag, (EXTRA, GW)))
    )
    return packed, off, extra


def curvature_kernel(groups_ref, counts_ref, eff_ref, nom_ref, obs_ref, var_ref, theta_ref, out_ref):
    chan = lax.axis_index("chan")
    bins = lax.axis_index("bins")
    c = pl.program_id(0)
    size = eff_ref.shape[1]
    base = chan * pl.num_programs(0) + c
    g0, g1 = groups_ref[base, 0], groups_ref[base, 1]
    chosen = jnp.concatenate([theta_ref[g0], theta_ref[g1]], axis=1).astype(jnp.bfloat16)
    chosen = jnp.broadcast_to(chosen, (16, 2 * GW))
    line = pl.ds(c, 1)
    nominal, observed, variance = nom_ref[line], obs_ref[line].astype(jnp.float32), var_ref[line]
    position = bins * size + lax.broadcasted_iota(jnp.int32, (8, size), 1)
    packed, off, extra = channel_payload(
        eff_ref[0], chosen, nominal, observed, variance, position < counts_ref[c]
    )
    out_ref[0, :GW] = packed
    out_ref[0, GW : 2 * GW] = off
    out_ref[0, 2 * GW :] = extra


def curvature(effects, nominal, observed, variance, theta, groups, counts):
    chans, size, width = effects.shape
    rows = 2 * GW + EXTRA
    whole = lambda *shape: pl.BlockSpec(shape, lambda c, *_: (0,) * len(shape))
    return pl.pallas_call(
        curvature_kernel,
        grid_spec=pltpu.PrefetchScalarGridSpec(
            num_scalar_prefetch=2,
            grid=(chans,),
            in_specs=[
                pl.BlockSpec((1, size, width), lambda c, *_: (c, 0, 0)),
                whole(chans, size),
                whole(chans, size),
                whole(chans, size),
                whole(theta.shape[0] // GW, 1, GW),
            ],
            out_specs=pl.BlockSpec((1, rows, GW), lambda c, *_: (c, 0, 0)),
        ),
        out_shape=jax.ShapeDtypeStruct((chans, rows, GW), jnp.float32),
        compiler_params=pltpu.CompilerParams(vmem_limit_bytes=58 * 2**20),
        name="curvature",
    )(
        groups,
        counts,
        effects,
        nominal,
        observed,
        variance,
        theta.reshape(-1, 1, GW),
    )


def place_kernel(
    groups_ref, owner_ref, payload_ref, theta_ref, tiles_ref, grad_ref,
    lookup, entries, counts,
):
    step = pl.program_id(0)
    slots = counts.shape[0] - 1
    device = lax.axis_index("chan") * lax.axis_size("bins") + lax.axis_index("bins")
    chans = payload_ref.shape[0]
    per_tile = TILE // GW
    total_groups = theta_ref.shape[0]
    side = total_groups // per_tile
    shift = per_tile.bit_length() - 1
    room = 4 * chans
    start = device * slots

    @pl.when(step == 0)
    def _():
        def clear(i, _):
            for j in range(16):
                lookup[i * 16 + j] = slots
            return 0

        lax.fori_loop(0, side * side // 16, clear, 0)
        counts[slots] = 0
        for s in range(slots):
            counts[s] = 0
            lookup[owner_ref[start + s]] = s

        def visit(pair, _):
            for c in (pair * 2, pair * 2 + 1):
                a, b = groups_ref[c, 0], groups_ref[c, 1]
                ta, tb = a >> shift, b >> shift
                ra, rb = a & (per_tile - 1), b & (per_tile - 1)
                cases = ((ta, ta, ra, ra), (tb, tb, rb, rb), (ta, tb, ra, rb), (tb, ta, rb, ra))
                for kind, (tr, tc, rr, rc) in enumerate(cases):
                    slot = lookup[tr * side + tc]
                    n = counts[slot]
                    entries[slot * room + n] = ((((c << shift) + rr) << shift) + rc) * 4 + kind
                    counts[slot] = n + 1
            return 0

        lax.fori_loop(0, chans // 2, visit, 0)

    tile = owner_ref[start + step]

    tiles_ref[...] = jnp.zeros_like(tiles_ref)
    eye = (
        lax.broadcasted_iota(jnp.int32, (GW, GW), 0) == lax.broadcasted_iota(jnp.int32, (GW, GW), 1)
    ).astype(jnp.float32)

    @pl.when(tile // side == tile % side)
    def _():
        for r in range(per_tile):
            tiles_ref[0, r * GW : (r + 1) * GW, r * GW : (r + 1) * GW] = eye

    row = lax.broadcasted_iota(jnp.int32, (GW, GW), 0)
    col = lax.broadcasted_iota(jnp.int32, (GW, GW), 1)

    def accumulate(i, _):
        code = entries[step * room + i]
        kind = code & 3
        rc = (code >> 2) & (per_tile - 1)
        rr = (code >> (2 + shift)) & (per_tile - 1)
        c = code >> (2 + 2 * shift)
        at = (
            0,
            pl.ds(pl.multiple_of(rr * GW, GW), GW),
            pl.ds(pl.multiple_of(rc * GW, GW), GW),
        )

        @pl.when(kind == 0)
        def _():
            upper = jnp.where(row <= col, payload_ref[c, :GW], 0.0)
            tiles_ref[at] += upper + jnp.where(row > col, upper.T, 0.0)

        @pl.when(kind == 1)
        def _():
            lower = jnp.where(row > col, payload_ref[c, :GW], 0.0)
            diag = jnp.where(row == col, payload_ref[c, 2 * GW + 2 : 2 * GW + 3], 0.0)
            tiles_ref[at] += lower + lower.T + diag

        @pl.when(kind == 2)
        def _():
            tiles_ref[at] += payload_ref[c, GW : 2 * GW]

        @pl.when(kind == 3)
        def _():
            tiles_ref[at] += payload_ref[c, GW : 2 * GW].T

        return 0

    lax.fori_loop(0, counts[step], accumulate, 0)

    @pl.when(step == slots - 1)
    def _():
        mine = grad_ref.shape[0]
        first = device * total_groups // (lax.axis_size("chan") * lax.axis_size("bins"))
        for m in range(mine):
            grad_ref[m] = theta_ref[first + m]

        def add(c, _):
            for r in range(2):
                m = groups_ref[c, r] - first

                @pl.when(jnp.logical_and(m >= 0, m < mine))
                def _(m=m, r=r):
                    grad_ref[m] += payload_ref[c, 2 * GW + r : 2 * GW + r + 1]

            return 0

        lax.fori_loop(0, chans, add, 0)


def place(payload, theta, groups, tile_owner, slots, mine):
    chans, rows = payload.shape[:2]
    return pl.pallas_call(
        place_kernel,
        grid_spec=pltpu.PrefetchScalarGridSpec(
            num_scalar_prefetch=2,
            grid=(slots,),
            in_specs=[
                pl.BlockSpec(memory_space=pltpu.VMEM),
                pl.BlockSpec((theta.shape[0] // GW, 1, GW), lambda s, *_: (0, 0, 0)),
            ],
            out_specs=[
                pl.BlockSpec((1, TILE, TILE), lambda s, *_: (s, 0, 0)),
                pl.BlockSpec((mine, 1, GW), lambda s, *_: (0, 0, 0)),
            ],
            scratch_shapes=[
                pltpu.SMEM((tile_owner.shape[0],), jnp.int32),
                pltpu.SMEM(((slots + 1) * chans * 4,), jnp.int32),
                pltpu.SMEM((slots + 1,), jnp.int32),
            ],
        ),
        out_shape=[
            jax.ShapeDtypeStruct((slots, TILE, TILE), jnp.float32),
            jax.ShapeDtypeStruct((mine, 1, GW), jnp.float32),
        ],
        compiler_params=pltpu.CompilerParams(
            vmem_limit_bytes=4 * chans * (rows + EXTRA) * GW + 8 * 2**20
        ),
        name="place",
    )(groups, tile_owner, payload, theta.reshape(-1, 1, GW))


COLORS = ((0, 112, "zxy"), (112, 88, "zyx"), (200, 64, "xyz"))
DEEP = 4
TOGETHER = 4
LINKS = 5


def exponent_rows(eff, chosen, nominal, observed, variance, live, left_ref):
    eff_t = eff.T
    exponent = jnp.dot(chosen, eff_t, preferred_element_type=jnp.float32)[0:8]
    expected = nominal * jnp.exp(exponent)
    denominator = 1.0 + expected * variance
    residual = jnp.where(live, (expected - observed) / denominator, 0.0)
    weight = jnp.where(live, expected / denominator, 0.0)
    left_ref[: 2 * GW] = (eff_t.astype(jnp.float32) * weight[0:1]).astype(jnp.bfloat16)
    left_ref[2 * GW :] = jnp.concatenate([residual, residual], axis=0).astype(jnp.bfloat16)


def block_rows(left, eff):
    full = jnp.dot(left, eff, preferred_element_type=jnp.float32)
    first, off, second = full[:GW, :GW], full[:GW, GW:], full[GW : 2 * GW, GW:]
    row = lax.broadcasted_iota(jnp.int32, (GW, GW), 0)
    col = lax.broadcasted_iota(jnp.int32, (GW, GW), 1)
    packed = jnp.where(row <= col, first, second)
    second_diag = jnp.sum(jnp.where(row == col, second, 0.0), axis=0, keepdims=True)
    grad0 = full[2 * GW : 2 * GW + 8, :GW]
    grad1 = full[2 * GW : 2 * GW + 8, GW:]
    which = lax.broadcasted_iota(jnp.int32, (EXTRA, GW), 0)
    extra = jnp.where(
        which == 0, grad0, jnp.where(which == 1, grad1, jnp.broadcast_to(second_diag, (EXTRA, GW)))
    )
    return packed, off, extra


def make_plan(index_ref, mine, total_groups, plan_ref):
    per_tile = TILE // GW
    shift = per_tile.bit_length() - 1
    side = total_groups // per_tile
    chans = index_ref.shape[0]
    slots = len(mine)
    count = 4 * chans
    gshift = GW.bit_length() - 1
    a, b = index_ref[:, :GW] >> gshift, index_ref[:, GW:] >> gshift
    ta, tb = a >> shift, b >> shift
    ra, rb = a & (per_tile - 1), b & (per_tile - 1)
    c = lax.broadcasted_iota(jnp.int32, (chans, GW), 0)
    keys, codes, places = [], [], []
    cases = ((ta, ta, ra, ra), (tb, tb, rb, rb), (ta, tb, ra, rb), (tb, ta, rb, ra))
    for kind, (tr, tc, rr, rc) in enumerate(cases):
        tile = tr * side + tc
        slot = jnp.full((chans, GW), slots, jnp.int32)
        for s in range(slots):
            slot = jnp.where(tile == mine[s], s, slot)
        places.append(slot)
        keys.append(slot * count + kind * chans + c)
        codes.append(((((c << shift) + rr) << shift) + rc) * 4 + kind)
    key = jnp.concatenate(keys, axis=0)
    code = jnp.concatenate(codes, axis=0).astype(jnp.float32)
    place_col = jnp.concatenate(places, axis=0)
    lane = lax.broadcasted_iota(jnp.int32, (count, GW), 1)
    key_rows = key.T
    rank = jnp.zeros((count, 1), jnp.float32)
    for j in range(0, count, GW):
        less = jnp.where(key_rows[0:1, j : j + GW] < key, 1.0, 0.0)
        rank += jnp.sum(less, axis=1, keepdims=True)
    rank = jnp.broadcast_to(rank, (count, GW)).astype(jnp.int32)
    for j in range(0, count, GW):
        picked = jnp.sum(jnp.where(rank == lane + j, code, 0.0), axis=0, keepdims=True)
        plan_ref[0:1, j : j + GW] = picked.astype(jnp.int32)
    starts = jnp.sum(jnp.where(place_col < lane, 1.0, 0.0), axis=0, keepdims=True)
    plan_ref[1:2, 0:GW] = starts.astype(jnp.int32)
    lane1 = lax.broadcasted_iota(jnp.int32, (1, GW), 1)
    diagonal = jnp.zeros((1, GW), jnp.int32)
    for s in range(slots):
        t = jnp.full((1, GW), mine[s], jnp.int32)
        on = (t >> (side.bit_length() - 1)) == (t & (side - 1))
        diagonal = jnp.where(jnp.logical_and(lane1 == s, on), 1, diagonal)
    plan_ref[2:3, 0:GW] = diagonal


def exchange_kernel(
    ydim, slots, index_hbm, counts_hbm, eff_hbm, nom_hbm, obs_hbm, var_hbm, theta_hbm, owner_hbm,
    out_ref, plan_ref,
    eff_held, parts_ref, swap, cross, total, left, nom_ref, obs_ref, var_ref, theta_ref, index_ref,
    local_index, counts_ref, owner_ref,
    eff_sem, small_sem, swap_recv, cross_recv, recv, drecv, send,
):
    chan, bins = lax.axis_index("chan"), lax.axis_index("bins")
    zdim = lax.axis_size("chan") // ydim
    nbins = lax.axis_size("bins")
    z, y = chan // ydim, chan % ydim
    x, core = bins // 2, bins % 2
    chans, size = eff_held.shape[:2]
    held = chans // nbins
    sent = {}
    colors = len(COLORS)

    def device(zz, yy, xx, kk):
        return {"chan": zz * ydim + yy, "bins": xx * 2 + kk}

    def run(cond, action):
        if cond is None:
            action()
        else:
            pl.when(cond)(action)

    def copy(src, dst, recv_sem, target, group, there=None):
        made = pltpu.make_async_remote_copy(
            src_ref=src,
            dst_ref=dst,
            send_sem=send.at[group],
            recv_sem=recv_sem,
            device_id=target,
            device_id_type=pl.DeviceIdType.MESH,
        )
        cond, places = (None, range(zdim)) if there is None else there
        counted = sent.setdefault(group, [0] * zdim)
        for place in places:
            counted[place] += 1
        run(cond, made.start)

    far, near = (1 - x) * 2, x * 2
    owners = (far + 1 - core, far + core, near + 1 - core, near + core)

    def load(q, h):
        at = q * held + h
        return pltpu.make_async_copy(eff_hbm.at[owners[q] * held + h], eff_held.at[at], eff_sem.at[at])

    mine_rows = pl.ds(pl.multiple_of(chan * chans, chans), chans)
    smalls = [
        (index_hbm.at[mine_rows], local_index),
        (counts_hbm, counts_ref),
        (theta_hbm, theta_ref),
        (nom_hbm, nom_ref),
        (var_hbm, var_ref),
        (obs_hbm, obs_ref),
        (owner_hbm, owner_ref),
        (index_hbm, index_ref),
    ]
    smalls = [pltpu.make_async_copy(a, b, small_sem.at[n]) for n, (a, b) in enumerate(smalls)]
    steps = [(q, h) for h in range(held) for q in range(4)]
    for made in smalls[:3]:
        made.start()
    load(*steps[0]).start()
    for made in smalls[3:6]:
        made.start()
    for step in steps[1:2]:
        load(*step).start()

    partner = device(z, y, x, 1 - core)
    beside = device(z, y, 1 - x, core)
    below_there, above_there = z > 0, z < zdim - 1

    barrier = pltpu.get_barrier_semaphore()
    for target, cond in (
        (partner, None),
        (beside, None),
        (device(z, 1 - y, x, core), None),
        (device(z - 1, y, x, core), below_there),
        (device(z + 1, y, x, core), above_there),
    ):
        run(cond, lambda target=target: pl.semaphore_signal(
            barrier, 1, device_id=target, device_id_type=pl.DeviceIdType.MESH
        ))
    for made in smalls[:6]:
        made.wait()

    def prepare(q, h):
        c = owners[q] * held + h
        g0 = local_index[c, 0] >> (GW.bit_length() - 1)
        g1 = local_index[c, GW] >> (GW.bit_length() - 1)
        chosen = jnp.concatenate([theta_ref[g0], theta_ref[g1]], axis=1).astype(jnp.bfloat16)
        chosen = jnp.broadcast_to(chosen, (16, 2 * GW))
        line = pl.ds(c, 1)
        position = bins * size + lax.broadcasted_iota(jnp.int32, (8, size), 1)
        exponent_rows(
            eff_held[q * held + h],
            chosen,
            nom_ref[line],
            obs_ref[line].astype(jnp.float32),
            var_ref[line],
            position < counts_ref[c],
            left.at[q % 2],
        )

    def multiply(q, h):
        packed, off, extra = block_rows(left[q % 2], eff_held[q * held + h])
        at = q * held + h
        parts_ref[at, :GW] = packed
        parts_ref[at, GW : 2 * GW] = off
        parts_ref[at, 2 * GW :] = extra

    def begin(n):
        load(*steps[n]).wait()
        if n + 2 < len(steps):
            load(*steps[n + 2]).start()
        if n == 2:
            for made in smalls[6:]:
                made.start()
        prepare(*steps[n])

    def compute(n):
        if n == 0:
            begin(0)
            multiply(*steps[0])
            return
        if n == 1:
            begin(1)
        if n + 1 < len(steps):
            begin(n + 1)
        multiply(*steps[n])

    def arrived(dst, sem):
        pltpu.make_async_remote_copy(
            src_ref=dst, dst_ref=dst, send_sem=send.at[0], recv_sem=sem,
            device_id=partner, device_id_type=pl.DeviceIdType.MESH,
        ).wait_recv()

    def to_partner(q, h):
        n = q // 2 * held + h
        copy(parts_ref.at[q * held + h], swap.at[n], swap_recv.at[n], partner, LINKS * colors)

    def send_across(h):
        arrived(swap.at[h], swap_recv.at[h])
        total[h] = parts_ref[held + h] + swap[h]
        for color, (first, count, _) in enumerate(COLORS):
            rows = pl.ds(first, count)
            copy(total.at[h, rows], cross.at[h, rows], cross_recv.at[h, color], beside, 2 * colors + color)

    own = (chan * nbins + bins) * held

    def finish(h, color):
        first, count, _ = COLORS[color]
        rows = pl.ds(first, count)
        arrived(cross.at[h, rows], cross_recv.at[h, color])
        out_ref[own + h, rows] = (
            parts_ref[3 * held + h, rows] + swap[held + h, rows]
        ) + cross[h, rows]

    def forward(h, color, dz, fx, fy):
        first, count, order = COLORS[color]
        sz, sx, sy = z + dz, (1 - x if fx else x), (1 - y if fy else y)
        chip = (sz * ydim + sy) * 2 + sx
        there = None if dz == 0 else (z >= -dz if dz < 0 else z < zdim - dz)
        places = [p for p in range(zdim) if 0 <= p + dz < zdim]
        at = ((sz * ydim + sy) * nbins + sx * 2 + core) * held + h
        piece = out_ref.at[at, pl.ds(first, count)]
        offset = {"z": dz, "x": fx, "y": fy}
        last = max([n for n, d in enumerate(order) if offset[d]], default=-1)
        sem = recv.at[h, color, chip]
        if last >= 0:
            run(there, lambda: arrived(piece, sem))

        def both(a, b):
            return b if a is None else (a if b is None else jnp.logical_and(a, b))

        here = (there, places)
        if zdim > 1:
            onward = order.index("z") > last
            if (onward or (last >= 0 and order[last] == "z" and dz < 0)) and dz >= 2 - zdim:
                up = (both(there, above_there), [p for p in places if p < zdim - 1])
                copy(piece, piece, sem, device(z + 1, y, x, core), color, up)
            if (onward or (last >= 0 and order[last] == "z" and dz > 0)) and dz <= zdim - 2:
                down = (both(there, below_there), [p for p in places if p > 0])
                copy(piece, piece, sem, device(z - 1, y, x, core), colors + color, down)
        if order.index("x") > last:
            copy(piece, piece, sem, beside, 2 * colors + color, here)
        if order.index("y") > last:
            copy(piece, piece, sem, device(z, 1 - y, x, core), 3 * colors + color, here)
        copy(piece, piece, drecv.at[color], partner, 4 * colors + color, here)

    compute(0)
    pl.semaphore_wait(barrier, 3 + jnp.minimum(z, 1) + jnp.minimum(zdim - 1 - z, 1))
    to_partner(0, 0)
    compute(1)
    send_across(0)
    compute(2)
    to_partner(2, 0)
    compute(3)
    compute(4)
    to_partner(0, 1)
    compute(5)
    send_across(1)
    arrived(swap.at[held], swap_recv.at[held])
    finish(0, 0)
    forward(0, 0, 0, 0, 0)
    compute(6)
    to_partner(2, 1)
    finish(0, 1)
    forward(0, 1, 0, 0, 0)
    compute(7)
    finish(0, 2)
    forward(0, 2, 0, 0, 0)
    arrived(swap.at[held + 1], swap_recv.at[held + 1])
    order = [e for e in ORDER if abs(e[2]) < zdim]
    for n, e in enumerate(order):
        if n == PLAN_AT:
            for made in smalls[6:]:
                made.wait()
            me = (chan * nbins + bins) * slots
            make_plan(
                index_ref, [owner_ref[me + s] for s in range(slots)], theta_ref.shape[0], plan_ref
            )
        h, color, dz, fx, fy = e
        if (dz, fx, fy) == (0, 0, 0):
            finish(h, color)
        forward(*e)

    chips = zdim * ydim * 2

    def waiting(n, count, group, color):
        part = out_ref.at[pl.ds(0, n), pl.ds(0, count)]
        return pltpu.make_async_remote_copy(
            src_ref=part, dst_ref=part, send_sem=send.at[group], recv_sem=drecv.at[color],
            device_id=partner, device_id_type=pl.DeviceIdType.MESH,
        )

    for color, (_, count, _) in enumerate(COLORS):
        waiting(held * chips, count, 0, color).wait_recv()
    for group, numbers in sent.items():
        count = COLORS[group % colors][1] if group < LINKS * colors else out_ref.shape[1]
        if len(set(numbers)) == 1:
            waiting(numbers[0], count, group, 0).wait_send()
            continue
        for place, number in enumerate(numbers):
            if number:
                pl.when(z == place)(waiting(number, count, group, 0).wait_send)


ORDER = (
    (1, 0, 0, 0, 0), (1, 1, 0, 0, 0), (1, 2, 0, 0, 0), (0, 0, -1, 0, 0), (0, 2, 0, 0, 1),
    (0, 0, 1, 0, 0), (1, 0, 1, 0, 0), (0, 1, 1, 0, 0), (1, 0, -1, 0, 0), (1, 1, 1, 0, 0),
    (1, 1, -1, 0, 0), (0, 2, 0, 1, 0), (0, 1, -1, 0, 0), (0, 0, 0, 1, 0), (1, 2, 0, 1, 0),
    (1, 0, 2, 0, 0), (1, 1, 0, 0, 1), (0, 1, 2, 0, 0), (1, 1, 2, 0, 0), (1, 1, -2, 0, 0),
    (0, 2, -1, 0, 0), (0, 1, -2, 0, 0), (1, 0, 0, 0, 1), (1, 2, -1, 1, 0), (0, 2, 1, 0, 0),
    (1, 0, -2, 0, 0), (1, 1, 0, 1, 0), (0, 0, 2, 0, 0), (1, 2, 1, 1, 0), (0, 1, 1, 0, 1),
    (0, 0, 1, 1, 0), (1, 1, -3, 0, 0), (1, 0, 1, 0, 1), (0, 1, 3, 0, 0), (0, 0, -2, 0, 0),
    (1, 0, 3, 0, 0), (1, 2, 0, 0, 1), (0, 2, 0, 1, 1), (1, 0, 0, 1, 0), (1, 2, 1, 0, 0),
    (1, 2, 1, 0, 1), (1, 1, 1, 1, 0), (1, 0, -3, 0, 0), (1, 2, 0, 1, 1), (1, 2, 2, 1, 0),
    (0, 0, -3, 0, 0), (0, 2, -1, 0, 1), (0, 2, -1, 1, 1), (0, 0, 3, 0, 0), (0, 1, 2, 0, 1),
    (0, 1, -3, 0, 0), (0, 2, -2, 0, 0), (1, 2, -1, 0, 0), (1, 1, 3, 0, 0), (0, 1, -2, 0, 1),
    (1, 0, -3, 1, 0), (0, 1, 0, 0, 1), (1, 0, 2, 1, 0), (0, 2, 1, 0, 1), (1, 1, 1, 0, 1),
    (1, 0, -1, 1, 0), (0, 1, -3, 0, 1), (0, 0, -1, 1, 0), (0, 2, 1, 1, 1), (0, 2, 1, 1, 0),
    (0, 0, 1, 0, 1), (1, 1, -1, 0, 1), (1, 0, 3, 1, 0), (1, 2, 1, 1, 1), (0, 2, -1, 1, 0),
    (0, 1, 1, 1, 0), (0, 2, 2, 0, 0), (1, 2, 2, 0, 1), (0, 0, 3, 0, 1), (0, 0, -3, 1, 0),
    (1, 2, 2, 0, 0), (1, 1, 2, 0, 1), (0, 0, 3, 1, 0), (1, 2, 3, 1, 0), (1, 2, -1, 0, 1),
    (1, 0, -1, 0, 1), (0, 2, -2, 0, 1), (0, 0, -2, 0, 1), (1, 1, -3, 0, 1), (1, 2, -1, 1, 1),
    (1, 0, 1, 1, 0), (1, 1, -2, 0, 1), (0, 0, 2, 1, 0), (1, 0, 3, 0, 1), (0, 2, -3, 0, 0),
    (0, 0, -3, 0, 1), (0, 2, 2, 1, 1), (0, 0, -1, 0, 1), (1, 1, 3, 0, 1), (0, 1, -1, 0, 1),
    (0, 2, -2, 1, 0), (0, 1, 2, 1, 0), (1, 0, -2, 1, 0), (1, 2, -2, 0, 1), (0, 2, 2, 0, 1),
    (1, 2, 2, 1, 1), (0, 0, -2, 1, 0), (1, 1, 3, 1, 0), (1, 2, -2, 1, 0), (1, 0, -3, 1, 1),
    (0, 1, 3, 0, 1), (1, 0, 0, 1, 1), (0, 2, -3, 1, 0), (1, 2, -2, 0, 0), (0, 2, -3, 0, 1),
    (1, 2, -3, 1, 0), (1, 2, -3, 1, 1), (1, 1, 3, 1, 1), (1, 2, -2, 1, 1), (1, 0, 2, 1, 1),
    (0, 1, 2, 1, 1), (0, 0, 1, 1, 1), (0, 2, 2, 1, 0), (0, 1, 0, 1, 1), (1, 1, 1, 1, 1),
    (1, 1, 2, 1, 1), (1, 0, -2, 0, 1), (0, 1, 3, 1, 0), (0, 0, 0, 0, 1), (1, 1, -3, 1, 0),
    (1, 1, 2, 1, 0), (1, 0, -3, 0, 1), (1, 1, -1, 1, 1), (0, 1, -2, 1, 1), (0, 2, 3, 0, 1),
    (1, 1, -2, 1, 0), (1, 1, 0, 1, 1), (1, 2, 3, 0, 1), (0, 2, 3, 0, 0), (0, 0, 2, 0, 1),
    (0, 1, 3, 1, 1), (0, 1, -1, 1, 0), (1, 2, -3, 0, 1), (1, 1, -3, 1, 1), (0, 0, -3, 1, 1),
    (0, 1, -3, 1, 1), (0, 2, -3, 1, 1), (1, 1, -1, 1, 0), (0, 1, 1, 1, 1), (0, 2, -2, 1, 1),
    (0, 0, 0, 1, 1), (1, 0, -1, 1, 1), (1, 0, 3, 1, 1), (0, 0, -1, 1, 1), (0, 0, 3, 1, 1),
    (1, 2, 3, 1, 1), (0, 2, 3, 1, 1), (1, 1, -2, 1, 1), (1, 0, 2, 0, 1), (0, 1, -3, 1, 0),
    (1, 2, 3, 0, 0), (0, 0, -2, 1, 1), (1, 0, 1, 1, 1), (0, 1, 0, 1, 0), (0, 0, 2, 1, 1),
    (0, 1, -2, 1, 0), (1, 2, -3, 0, 0), (1, 0, -2, 1, 1), (0, 2, 3, 1, 0), (0, 1, -1, 1, 1),
)
PLAN_AT = 0


def exchange(effects, nominal, observed, variance, theta, nuisance_index, counts, tile_owner):
    nbins, nchan = lax.axis_size("bins"), lax.axis_size("chan")
    chans, size, channel_width = effects.shape
    rows, width = 2 * GW + EXTRA, GW
    held = chans // nbins
    hbm = pl.BlockSpec(memory_space=pltpu.HBM)
    vmem = pl.BlockSpec(memory_space=pltpu.VMEM)
    chips = nchan * nbins // 2
    slots = tile_owner.shape[0] // (nchan * nbins)
    colors = len(COLORS)
    operands = (
        nuisance_index, counts, effects, nominal, observed, variance,
        theta.reshape(-1, 1, GW), tile_owner,
    )
    return pl.pallas_call(
        functools.partial(exchange_kernel, 2, slots),
        in_specs=[hbm] * len(operands),
        out_specs=[vmem, vmem],
        out_shape=[
            jax.ShapeDtypeStruct((nchan * chans, rows, width), jnp.float32),
            jax.ShapeDtypeStruct((8, 4 * nchan * chans), jnp.int32),
        ],
        scratch_shapes=[
            pltpu.VMEM((chans, size, channel_width), jnp.bfloat16),
            pltpu.VMEM((chans, rows, width), jnp.float32),
            pltpu.VMEM((2 * held, rows, width), jnp.float32),
            pltpu.VMEM((held, rows, width), jnp.float32),
            pltpu.VMEM((held, rows, width), jnp.float32),
            pltpu.VMEM((2, channel_width + 16, size), jnp.bfloat16),
            pltpu.VMEM(nominal.shape, nominal.dtype),
            pltpu.VMEM(observed.shape, observed.dtype),
            pltpu.VMEM(variance.shape, variance.dtype),
            pltpu.VMEM((theta.shape[0] // GW, 1, GW), theta.dtype),
            pltpu.VMEM(nuisance_index.shape, jnp.int32),
            pltpu.SMEM((chans, nuisance_index.shape[1]), jnp.int32),
            pltpu.SMEM(counts.shape, jnp.int32),
            pltpu.SMEM(tile_owner.shape, jnp.int32),
            pltpu.SemaphoreType.DMA((chans,)),
            pltpu.SemaphoreType.DMA((8,)),
            pltpu.SemaphoreType.DMA((2 * held,)),
            pltpu.SemaphoreType.DMA((held, colors)),
            pltpu.SemaphoreType.DMA((held, colors, chips)),
            pltpu.SemaphoreType.DMA((colors,)),
            pltpu.SemaphoreType.DMA((LINKS * colors + 1,)),
        ],
        compiler_params=pltpu.CompilerParams(
            collective_id=0, has_side_effects=True, vmem_limit_bytes=32 * 2**20
        ),
        name="exchange",
    )(*[pltpu.with_memory_space_constraint(a, pltpu.HBM) for a in operands])


def fill_kernel(
    plan_hbm, payload_ref, index_ref, theta_ref, tiles_ref, grad_hbm,
    plan_ref, grad_ref, held_tiles, sems, small_sems,
):
    slots = held_tiles.shape[0]
    per_tile = TILE // GW
    shift = per_tile.bit_length() - 1
    row = lax.broadcasted_iota(jnp.int32, (GW, GW), 0)
    col = lax.broadcasted_iota(jnp.int32, (GW, GW), 1)
    eye = (row == col).astype(jnp.float32)
    ahead = min(2, slots)

    get_plan = pltpu.make_async_copy(plan_hbm, plan_ref, small_sems.at[0])
    put_grad = pltpu.make_async_copy(grad_ref, grad_hbm, small_sems.at[1])
    get_plan.start()

    def put(s):
        return pltpu.make_async_copy(held_tiles.at[s], tiles_ref.at[s], sems.at[s])

    def clear(s):
        held_tiles[s] = jnp.zeros((TILE, TILE), jnp.float32)

    for s in range(ahead):
        clear(s)

    mine = grad_ref.shape[0]
    device = lax.axis_index("chan") * lax.axis_size("bins") + lax.axis_index("bins")
    total_groups = theta_ref.shape[0]
    first = device * total_groups // (lax.axis_size("chan") * lax.axis_size("bins"))
    gshift = GW.bit_length() - 1
    for m in range(mine):
        acc = theta_ref[first + m]
        for r in range(2):
            hit = (index_ref[:, r * GW : (r + 1) * GW] >> gshift) == first + m
            acc += jnp.sum(jnp.where(hit, payload_ref[:, 2 * GW + r], 0.0), axis=0, keepdims=True)
        grad_ref[m] = acc
    put_grad.start()
    get_plan.wait()

    def one_tile(s, _):
        @pl.when(plan_ref[2, s] == 1)
        def _():
            for r in range(per_tile):
                held_tiles[s, r * GW : (r + 1) * GW, r * GW : (r + 1) * GW] = eye

        start, end = plan_ref[1, s], plan_ref[1, s + 1]

        def block_of(i):
            valid = i < end
            code = plan_ref[0, jnp.minimum(i, end - 1)]
            kind = code & 3
            rc = (code >> 2) & (per_tile - 1)
            rr = (code >> (2 + shift)) & (per_tile - 1)
            c = code >> (2 + 2 * shift)
            block = payload_ref[c, pl.ds(pl.multiple_of((kind >> 1) * GW, GW), GW)]
            side = jnp.where(kind == 0, row - col, jnp.where(kind == 1, col - row, kind - 2))
            value = jnp.where(side > 0, block.T, block)
            diag = payload_ref[c, 2 * GW + 2 : 2 * GW + 3]
            value = jnp.where(jnp.logical_and(kind == 1, row == col), diag, value)
            at = (
                s,
                pl.ds(pl.multiple_of(rr * GW, GW), GW),
                pl.ds(pl.multiple_of(rc * GW, GW), GW),
            )
            return at, jnp.where(valid, value, 0.0)

        def accumulate(i, _):
            for at, value in [block_of(start + i * TOGETHER + j) for j in range(TOGETHER)]:
                held_tiles[at] += value
            return 0

        lax.fori_loop(0, (end - start + TOGETHER - 1) // TOGETHER, accumulate, 0)
        put(s).start()

        @pl.when(s + ahead < slots)
        def _():
            clear(s + ahead)

        return 0

    lax.fori_loop(0, slots, one_tile, 0)

    def drain(s, _):
        put(s).wait()
        return 0

    lax.fori_loop(0, slots, drain, 0)
    put_grad.wait()


def fill(payload, plan, theta, nuisance_index, slots, mine):
    chans, rows = payload.shape[:2]
    vmem = pl.BlockSpec(memory_space=pltpu.VMEM)
    hbm = pl.BlockSpec(memory_space=pltpu.HBM)
    return pl.pallas_call(
        fill_kernel,
        in_specs=[vmem, vmem, vmem, vmem],
        out_specs=[hbm, hbm],
        out_shape=[
            jax.ShapeDtypeStruct((slots, TILE, TILE), jnp.float32),
            jax.ShapeDtypeStruct((mine, 1, GW), jnp.float32),
        ],
        scratch_shapes=[
            pltpu.SMEM(plan.shape, plan.dtype),
            pltpu.VMEM((mine, 1, GW), jnp.float32),
            pltpu.VMEM((slots, TILE, TILE), jnp.float32),
            pltpu.SemaphoreType.DMA((slots,)),
            pltpu.SemaphoreType.DMA((2,)),
        ],
        compiler_params=pltpu.CompilerParams(
            vmem_limit_bytes=4 * chans * (rows + EXTRA) * GW + 4 * slots * TILE * TILE + 4 * 2**20
        ),
        name="fill",
    )(plan, payload, nuisance_index, theta.reshape(-1, 1, GW))


def local(effects, nominal, observed, mc_variance, theta, nuisance_index, bin_counts, tile_owner):
    devices = lax.axis_size("chan") * lax.axis_size("bins")
    device = lax.axis_index("chan") * lax.axis_size("bins") + lax.axis_index("bins")
    total_nu = theta.shape[0]
    slice_len = total_nu // devices
    slots, mine = tile_owner.shape[0] // devices, max(1, slice_len // GW)
    chan_size, bins_size = lax.axis_size("chan"), lax.axis_size("bins")
    if bins_size == 4 and chan_size % 2 == 0 and chan_size // 2 <= DEEP and effects.shape[0] == 2 * bins_size and slice_len >= GW:
        payload, plan = exchange(
            effects, nominal, observed, mc_variance, theta, nuisance_index, bin_counts, tile_owner
        )
        tiles, grad = fill(payload, plan, theta, nuisance_index, slots, mine)
    else:
        groups = nuisance_index[:, ::GW] // GW
        arrays = (effects, nominal, observed, mc_variance, theta, groups, bin_counts)
        summed = lax.psum_scatter(curvature(*arrays), "bins", scatter_dimension=0, tiled=True)
        payload = lax.all_gather(summed, ("chan", "bins"), axis=0, tiled=True)
        tiles, grad = place(payload, theta, groups, tile_owner, slots, mine)
    gradient = grad.reshape(-1)
    if slice_len < GW:
        gradient = lax.dynamic_slice_in_dim(gradient, device * slice_len % GW, slice_len, 0)
    return (tiles, gradient)


def solution(mesh):
    return jax.shard_map(
        local,
        mesh=mesh,
        in_specs=(
            P("chan", "bins", None),
            P("chan", "bins"),
            P("chan", "bins"),
            P("chan", "bins"),
            P(),
            P(),
            P("chan"),
            P(),
        ),
        out_specs=(P(("chan", "bins"), None, None), P(("chan", "bins"))),
        check_vma=False,
    )
```

```python
import functools

import jax
import jax.numpy as jnp
from jax import lax
from jax.experimental import pallas as pl
from jax.experimental.pallas import tpu as pltpu
from jax.sharding import PartitionSpec as P

GW = 128
TILE = 512
EXTRA = 8


def channel_payload(eff, chosen, nominal, observed, variance, live):
    eff_t = eff.T
    exponent = jnp.dot(chosen, eff_t, preferred_element_type=jnp.float32)[0:8]
    expected = nominal * jnp.exp(exponent)
    denominator = 1.0 + expected * variance
    residual = jnp.where(live, (expected - observed) / denominator, 0.0)
    weight = jnp.where(live, expected / denominator, 0.0)
    weighted = (eff_t.astype(jnp.float32) * weight[0:1]).astype(jnp.bfloat16)
    residual_rows = jnp.concatenate([residual, residual], axis=0).astype(jnp.bfloat16)
    left = jnp.concatenate([weighted, residual_rows], axis=0)
    full = jnp.dot(left, eff, preferred_element_type=jnp.float32)
    first, off, second = full[:GW, :GW], full[:GW, GW:], full[GW : 2 * GW, GW:]
    row = lax.broadcasted_iota(jnp.int32, (GW, GW), 0)
    col = lax.broadcasted_iota(jnp.int32, (GW, GW), 1)
    packed = jnp.where(row <= col, first, second)
    second_diag = jnp.sum(jnp.where(row == col, second, 0.0), axis=0, keepdims=True)
    grad0 = full[2 * GW : 2 * GW + 8, :GW]
    grad1 = full[2 * GW : 2 * GW + 8, GW:]
    which = lax.broadcasted_iota(jnp.int32, (EXTRA, GW), 0)
    extra = jnp.where(
        which == 0, grad0, jnp.where(which == 1, grad1, jnp.broadcast_to(second_diag, (EXTRA, GW)))
    )
    return packed, off, extra


def curvature_kernel(groups_ref, counts_ref, eff_ref, nom_ref, obs_ref, var_ref, theta_ref, out_ref):
    chan = lax.axis_index("chan")
    bins = lax.axis_index("bins")
    c = pl.program_id(0)
    size = eff_ref.shape[1]
    base = chan * pl.num_programs(0) + c
    g0, g1 = groups_ref[base, 0], groups_ref[base, 1]
    chosen = jnp.concatenate([theta_ref[g0], theta_ref[g1]], axis=1).astype(jnp.bfloat16)
    chosen = jnp.broadcast_to(chosen, (16, 2 * GW))
    line = pl.ds(c, 1)
    nominal, observed, variance = nom_ref[line], obs_ref[line].astype(jnp.float32), var_ref[line]
    position = bins * size + lax.broadcasted_iota(jnp.int32, (8, size), 1)
    packed, off, extra = channel_payload(
        eff_ref[0], chosen, nominal, observed, variance, position < counts_ref[c]
    )
    out_ref[0, :GW] = packed
    out_ref[0, GW : 2 * GW] = off
    out_ref[0, 2 * GW :] = extra


def curvature(effects, nominal, observed, variance, theta, groups, counts):
    chans, size, width = effects.shape
    rows = 2 * GW + EXTRA
    whole = lambda *shape: pl.BlockSpec(shape, lambda c, *_: (0,) * len(shape))
    return pl.pallas_call(
        curvature_kernel,
        grid_spec=pltpu.PrefetchScalarGridSpec(
            num_scalar_prefetch=2,
            grid=(chans,),
            in_specs=[
                pl.BlockSpec((1, size, width), lambda c, *_: (c, 0, 0)),
                whole(chans, size),
                whole(chans, size),
                whole(chans, size),
                whole(theta.shape[0] // GW, 1, GW),
            ],
            out_specs=pl.BlockSpec((1, rows, GW), lambda c, *_: (c, 0, 0)),
        ),
        out_shape=jax.ShapeDtypeStruct((chans, rows, GW), jnp.float32),
        compiler_params=pltpu.CompilerParams(vmem_limit_bytes=58 * 2**20),
        name="curvature",
    )(
        groups,
        counts,
        effects,
        nominal,
        observed,
        variance,
        theta.reshape(-1, 1, GW),
    )


def place_kernel(
    groups_ref, owner_ref, payload_ref, theta_ref, tiles_ref, grad_ref,
    lookup, entries, counts,
):
    step = pl.program_id(0)
    slots = counts.shape[0] - 1
    device = lax.axis_index("chan") * lax.axis_size("bins") + lax.axis_index("bins")
    chans = payload_ref.shape[0]
    per_tile = TILE // GW
    total_groups = theta_ref.shape[0]
    side = total_groups // per_tile
    shift = per_tile.bit_length() - 1
    room = 4 * chans
    start = device * slots

    @pl.when(step == 0)
    def _():
        def clear(i, _):
            for j in range(16):
                lookup[i * 16 + j] = slots
            return 0

        lax.fori_loop(0, side * side // 16, clear, 0)
        counts[slots] = 0
        for s in range(slots):
            counts[s] = 0
            lookup[owner_ref[start + s]] = s

        def visit(pair, _):
            for c in (pair * 2, pair * 2 + 1):
                a, b = groups_ref[c, 0], groups_ref[c, 1]
                ta, tb = a >> shift, b >> shift
                ra, rb = a & (per_tile - 1), b & (per_tile - 1)
                cases = ((ta, ta, ra, ra), (tb, tb, rb, rb), (ta, tb, ra, rb), (tb, ta, rb, ra))
                for kind, (tr, tc, rr, rc) in enumerate(cases):
                    slot = lookup[tr * side + tc]
                    n = counts[slot]
                    entries[slot * room + n] = ((((c << shift) + rr) << shift) + rc) * 4 + kind
                    counts[slot] = n + 1
            return 0

        lax.fori_loop(0, chans // 2, visit, 0)

    tile = owner_ref[start + step]

    tiles_ref[...] = jnp.zeros_like(tiles_ref)
    eye = (
        lax.broadcasted_iota(jnp.int32, (GW, GW), 0) == lax.broadcasted_iota(jnp.int32, (GW, GW), 1)
    ).astype(jnp.float32)

    @pl.when(tile // side == tile % side)
    def _():
        for r in range(per_tile):
            tiles_ref[0, r * GW : (r + 1) * GW, r * GW : (r + 1) * GW] = eye

    row = lax.broadcasted_iota(jnp.int32, (GW, GW), 0)
    col = lax.broadcasted_iota(jnp.int32, (GW, GW), 1)

    def accumulate(i, _):
        code = entries[step * room + i]
        kind = code & 3
        rc = (code >> 2) & (per_tile - 1)
        rr = (code >> (2 + shift)) & (per_tile - 1)
        c = code >> (2 + 2 * shift)
        at = (
            0,
            pl.ds(pl.multiple_of(rr * GW, GW), GW),
            pl.ds(pl.multiple_of(rc * GW, GW), GW),
        )

        @pl.when(kind == 0)
        def _():
            upper = jnp.where(row <= col, payload_ref[c, :GW], 0.0)
            tiles_ref[at] += upper + jnp.where(row > col, upper.T, 0.0)

        @pl.when(kind == 1)
        def _():
            lower = jnp.where(row > col, payload_ref[c, :GW], 0.0)
            diag = jnp.where(row == col, payload_ref[c, 2 * GW + 2 : 2 * GW + 3], 0.0)
            tiles_ref[at] += lower + lower.T + diag

        @pl.when(kind == 2)
        def _():
            tiles_ref[at] += payload_ref[c, GW : 2 * GW]

        @pl.when(kind == 3)
        def _():
            tiles_ref[at] += payload_ref[c, GW : 2 * GW].T

        return 0

    lax.fori_loop(0, counts[step], accumulate, 0)

    @pl.when(step == slots - 1)
    def _():
        mine = grad_ref.shape[0]
        first = device * total_groups // (lax.axis_size("chan") * lax.axis_size("bins"))
        for m in range(mine):
            grad_ref[m] = theta_ref[first + m]

        def add(c, _):
            for r in range(2):
                m = groups_ref[c, r] - first

                @pl.when(jnp.logical_and(m >= 0, m < mine))
                def _(m=m, r=r):
                    grad_ref[m] += payload_ref[c, 2 * GW + r : 2 * GW + r + 1]

            return 0

        lax.fori_loop(0, chans, add, 0)


def place(payload, theta, groups, tile_owner, slots, mine):
    chans, rows = payload.shape[:2]
    return pl.pallas_call(
        place_kernel,
        grid_spec=pltpu.PrefetchScalarGridSpec(
            num_scalar_prefetch=2,
            grid=(slots,),
            in_specs=[
                pl.BlockSpec(memory_space=pltpu.VMEM),
                pl.BlockSpec((theta.shape[0] // GW, 1, GW), lambda s, *_: (0, 0, 0)),
            ],
            out_specs=[
                pl.BlockSpec((1, TILE, TILE), lambda s, *_: (s, 0, 0)),
                pl.BlockSpec((mine, 1, GW), lambda s, *_: (0, 0, 0)),
            ],
            scratch_shapes=[
                pltpu.SMEM((tile_owner.shape[0],), jnp.int32),
                pltpu.SMEM(((slots + 1) * chans * 4,), jnp.int32),
                pltpu.SMEM((slots + 1,), jnp.int32),
            ],
        ),
        out_shape=[
            jax.ShapeDtypeStruct((slots, TILE, TILE), jnp.float32),
            jax.ShapeDtypeStruct((mine, 1, GW), jnp.float32),
        ],
        compiler_params=pltpu.CompilerParams(
            vmem_limit_bytes=4 * chans * (rows + EXTRA) * GW + 8 * 2**20
        ),
        name="place",
    )(groups, tile_owner, payload, theta.reshape(-1, 1, GW))


COLORS = ((0, 112, "zxy"), (112, 88, "zyx"), (200, 64, "xyz"))
DEEP = 4
PIECE = 512
TOGETHER = 4
LINKS = 5


def exponent_rows(eff_ref, chosen, nominal, observed, variance, live, left_ref, start, piece):
    at = slice(start, start + piece)
    eff_t = eff_ref[at].T
    exponent = jnp.dot(chosen, eff_t, preferred_element_type=jnp.float32)[0:8]
    expected = nominal[:, at] * jnp.exp(exponent)
    denominator = 1.0 + expected * variance[:, at]
    here = live[:, at]
    residual = jnp.where(here, (expected - observed[:, at]) / denominator, 0.0)
    weight = jnp.where(here, expected / denominator, 0.0)
    left_ref[: 2 * GW, at] = (eff_t.astype(jnp.float32) * weight[0:1]).astype(jnp.bfloat16)
    left_ref[2 * GW :, at] = jnp.concatenate([residual, residual], axis=0).astype(jnp.bfloat16)


def block_rows(full):
    first, off, second = full[:GW, :GW], full[:GW, GW:], full[GW : 2 * GW, GW:]
    row = lax.broadcasted_iota(jnp.int32, (GW, GW), 0)
    col = lax.broadcasted_iota(jnp.int32, (GW, GW), 1)
    packed = jnp.where(row <= col, first, second)
    second_diag = jnp.sum(jnp.where(row == col, second, 0.0), axis=0, keepdims=True)
    grad0 = full[2 * GW : 2 * GW + 8, :GW]
    grad1 = full[2 * GW : 2 * GW + 8, GW:]
    which = lax.broadcasted_iota(jnp.int32, (EXTRA, GW), 0)
    extra = jnp.where(
        which == 0, grad0, jnp.where(which == 1, grad1, jnp.broadcast_to(second_diag, (EXTRA, GW)))
    )
    return packed, off, extra


def make_plan(index_ref, mine, total_groups, plan_ref):
    per_tile = TILE // GW
    shift = per_tile.bit_length() - 1
    side = total_groups // per_tile
    chans = index_ref.shape[0]
    slots = len(mine)
    count = 4 * chans
    gshift = GW.bit_length() - 1
    a, b = index_ref[:, :GW] >> gshift, index_ref[:, GW:] >> gshift
    ta, tb = a >> shift, b >> shift
    ra, rb = a & (per_tile - 1), b & (per_tile - 1)
    c = lax.broadcasted_iota(jnp.int32, (chans, GW), 0)
    keys, codes, places = [], [], []
    cases = ((ta, ta, ra, ra), (tb, tb, rb, rb), (ta, tb, ra, rb), (tb, ta, rb, ra))
    for kind, (tr, tc, rr, rc) in enumerate(cases):
        tile = tr * side + tc
        slot = jnp.full((chans, GW), slots, jnp.int32)
        for s in range(slots):
            slot = jnp.where(tile == mine[s], s, slot)
        places.append(slot)
        keys.append(slot * count + kind * chans + c)
        codes.append(((((c << shift) + rr) << shift) + rc) * 4 + kind)
    key = jnp.concatenate(keys, axis=0)
    code = jnp.concatenate(codes, axis=0).astype(jnp.float32)
    place_col = jnp.concatenate(places, axis=0)
    lane = lax.broadcasted_iota(jnp.int32, (count, GW), 1)
    key_rows = key.T
    rank = jnp.zeros((count, 1), jnp.float32)
    for j in range(0, count, GW):
        less = jnp.where(key_rows[0:1, j : j + GW] < key, 1.0, 0.0)
        rank += jnp.sum(less, axis=1, keepdims=True)
    rank = jnp.broadcast_to(rank, (count, GW)).astype(jnp.int32)
    for j in range(0, count, GW):
        picked = jnp.sum(jnp.where(rank == lane + j, code, 0.0), axis=0, keepdims=True)
        plan_ref[0:1, j : j + GW] = picked.astype(jnp.int32)
    starts = jnp.sum(jnp.where(place_col < lane, 1.0, 0.0), axis=0, keepdims=True)
    plan_ref[1:2, 0:GW] = starts.astype(jnp.int32)
    lane1 = lax.broadcasted_iota(jnp.int32, (1, GW), 1)
    diagonal = jnp.zeros((1, GW), jnp.int32)
    for s in range(slots):
        t = jnp.full((1, GW), mine[s], jnp.int32)
        on = (t >> (side.bit_length() - 1)) == (t & (side - 1))
        diagonal = jnp.where(jnp.logical_and(lane1 == s, on), 1, diagonal)
    plan_ref[2:3, 0:GW] = diagonal


def exchange_kernel(
    ydim, slots, index_hbm, counts_hbm, eff_hbm, nom_hbm, obs_hbm, var_hbm, theta_hbm, owner_hbm,
    out_ref, plan_ref,
    eff_held, parts_ref, swap, cross, total, left, nom_ref, obs_ref, var_ref, theta_ref, index_ref,
    local_index, counts_ref, owner_ref,
    eff_sem, small_sem, swap_recv, cross_recv, recv, drecv, send,
):
    chan, bins = lax.axis_index("chan"), lax.axis_index("bins")
    zdim = lax.axis_size("chan") // ydim
    nbins = lax.axis_size("bins")
    z, y = chan // ydim, chan % ydim
    x, core = bins // 2, bins % 2
    chans, size = eff_held.shape[:2]
    held = chans // nbins
    sent = {}
    colors = len(COLORS)

    def device(zz, yy, xx, kk):
        return {"chan": zz * ydim + yy, "bins": xx * 2 + kk}

    def run(cond, action):
        if cond is None:
            action()
        else:
            pl.when(cond)(action)

    def copy(src, dst, recv_sem, target, group, there=None):
        made = pltpu.make_async_remote_copy(
            src_ref=src,
            dst_ref=dst,
            send_sem=send.at[group],
            recv_sem=recv_sem,
            device_id=target,
            device_id_type=pl.DeviceIdType.MESH,
        )
        cond, places = (None, range(zdim)) if there is None else there
        counted = sent.setdefault(group, [0] * zdim)
        for place in places:
            counted[place] += 1
        run(cond, made.start)

    far, near = (1 - x) * 2, x * 2
    owners = (far + 1 - core, far + core, near + 1 - core, near + core)

    def load(q, h):
        at = q * held + h
        return pltpu.make_async_copy(eff_hbm.at[owners[q] * held + h], eff_held.at[at], eff_sem.at[at])

    mine_rows = pl.ds(pl.multiple_of(chan * chans, chans), chans)
    smalls = [
        (index_hbm.at[mine_rows], local_index),
        (counts_hbm, counts_ref),
        (theta_hbm, theta_ref),
        (nom_hbm, nom_ref),
        (var_hbm, var_ref),
        (obs_hbm, obs_ref),
        (owner_hbm, owner_ref),
        (index_hbm, index_ref),
    ]
    smalls = [pltpu.make_async_copy(a, b, small_sem.at[n]) for n, (a, b) in enumerate(smalls)]
    steps = [(q, h) for h in range(held) for q in range(4)]
    for made in smalls[:3]:
        made.start()
    load(*steps[0]).start()
    for made in smalls[3:6]:
        made.start()
    for step in steps[1:2]:
        load(*step).start()

    partner = device(z, y, x, 1 - core)
    beside = device(z, y, 1 - x, core)
    below_there, above_there = z > 0, z < zdim - 1

    barrier = pltpu.get_barrier_semaphore()
    for target, cond in (
        (partner, None),
        (beside, None),
        (device(z, 1 - y, x, core), None),
        (device(z - 1, y, x, core), below_there),
        (device(z + 1, y, x, core), above_there),
    ):
        run(cond, lambda target=target: pl.semaphore_signal(
            barrier, 1, device_id=target, device_id_type=pl.DeviceIdType.MESH
        ))
    for made in smalls[:6]:
        made.wait()

    piece = min(PIECE, size)

    def prepare(q, h, start):
        c = owners[q] * held + h
        g0 = local_index[c, 0] >> (GW.bit_length() - 1)
        g1 = local_index[c, GW] >> (GW.bit_length() - 1)
        chosen = jnp.concatenate([theta_ref[g0], theta_ref[g1]], axis=1).astype(jnp.bfloat16)
        chosen = jnp.broadcast_to(chosen, (16, 2 * GW))
        line = pl.ds(c, 1)
        position = bins * size + lax.broadcasted_iota(jnp.int32, (8, size), 1)
        exponent_rows(
            eff_held.at[q * held + h],
            chosen,
            nom_ref[line],
            obs_ref[line].astype(jnp.float32),
            var_ref[line],
            position < counts_ref[c],
            left.at[q % 2],
            start,
            piece,
        )

    def begin(n):
        load(*steps[n]).wait()
        if n + 2 < len(steps):
            load(*steps[n + 2]).start()
        if n == 2:
            for made in smalls[6:]:
                made.start()

    def run_stage(first, second):
        if second is not None:
            begin(second)
        full = None
        for start in range(0, size, piece):
            if first is not None:
                q, h = steps[first]
                at = slice(start, start + piece)
                part = jnp.dot(
                    left[q % 2, :, at], eff_held[q * held + h, at],
                    preferred_element_type=jnp.float32,
                )
                full = part if full is None else full + part
            if second is not None:
                prepare(*steps[second], start)
        if first is not None:
            packed, off, extra = block_rows(full)
            parts_ref[q * held + h, :GW] = packed
            parts_ref[q * held + h, GW : 2 * GW] = off
            parts_ref[q * held + h, 2 * GW :] = extra

    def compute(n):
        if n < 2:
            run_stage(None, n)
        later = n + 1 if 0 < n < len(steps) - 1 else None
        run_stage(n, later)

    def arrived(dst, sem):
        pltpu.make_async_remote_copy(
            src_ref=dst, dst_ref=dst, send_sem=send.at[0], recv_sem=sem,
            device_id=partner, device_id_type=pl.DeviceIdType.MESH,
        ).wait_recv()

    def to_partner(q, h):
        n = q // 2 * held + h
        copy(parts_ref.at[q * held + h], swap.at[n], swap_recv.at[n], partner, LINKS * colors)

    def send_across(h):
        arrived(swap.at[h], swap_recv.at[h])
        total[h] = parts_ref[held + h] + swap[h]
        for color, (first, count, _) in enumerate(COLORS):
            rows = pl.ds(first, count)
            copy(total.at[h, rows], cross.at[h, rows], cross_recv.at[h, color], beside, 2 * colors + color)

    own = (chan * nbins + bins) * held

    def finish(h, color):
        first, count, _ = COLORS[color]
        rows = pl.ds(first, count)
        arrived(cross.at[h, rows], cross_recv.at[h, color])
        out_ref[own + h, rows] = (
            parts_ref[3 * held + h, rows] + swap[held + h, rows]
        ) + cross[h, rows]

    def forward(h, color, dz, fx, fy):
        first, count, order = COLORS[color]
        sz, sx, sy = z + dz, (1 - x if fx else x), (1 - y if fy else y)
        chip = (sz * ydim + sy) * 2 + sx
        there = None if dz == 0 else (z >= -dz if dz < 0 else z < zdim - dz)
        places = [p for p in range(zdim) if 0 <= p + dz < zdim]
        at = ((sz * ydim + sy) * nbins + sx * 2 + core) * held + h
        piece = out_ref.at[at, pl.ds(first, count)]
        offset = {"z": dz, "x": fx, "y": fy}
        last = max([n for n, d in enumerate(order) if offset[d]], default=-1)
        sem = recv.at[h, color, chip]
        if last >= 0:
            run(there, lambda: arrived(piece, sem))

        def both(a, b):
            return b if a is None else (a if b is None else jnp.logical_and(a, b))

        here = (there, places)
        if zdim > 1:
            onward = order.index("z") > last
            if (onward or (last >= 0 and order[last] == "z" and dz < 0)) and dz >= 2 - zdim:
                up = (both(there, above_there), [p for p in places if p < zdim - 1])
                copy(piece, piece, sem, device(z + 1, y, x, core), color, up)
            if (onward or (last >= 0 and order[last] == "z" and dz > 0)) and dz <= zdim - 2:
                down = (both(there, below_there), [p for p in places if p > 0])
                copy(piece, piece, sem, device(z - 1, y, x, core), colors + color, down)
        if order.index("x") > last:
            copy(piece, piece, sem, beside, 2 * colors + color, here)
        if order.index("y") > last:
            copy(piece, piece, sem, device(z, 1 - y, x, core), 3 * colors + color, here)
        copy(piece, piece, drecv.at[color], partner, 4 * colors + color, here)

    compute(0)
    pl.semaphore_wait(barrier, 3 + jnp.minimum(z, 1) + jnp.minimum(zdim - 1 - z, 1))
    to_partner(0, 0)
    compute(1)
    send_across(0)
    compute(2)
    to_partner(2, 0)
    compute(3)
    compute(4)
    to_partner(0, 1)
    compute(5)
    send_across(1)
    arrived(swap.at[held], swap_recv.at[held])
    finish(0, 0)
    forward(0, 0, 0, 0, 0)
    compute(6)
    to_partner(2, 1)
    finish(0, 1)
    forward(0, 1, 0, 0, 0)
    compute(7)
    finish(0, 2)
    forward(0, 2, 0, 0, 0)
    arrived(swap.at[held + 1], swap_recv.at[held + 1])
    order = [e for e in ORDER if abs(e[2]) < zdim]
    for n, e in enumerate(order):
        if n == PLAN_AT:
            for made in smalls[6:]:
                made.wait()
            me = (chan * nbins + bins) * slots
            make_plan(
                index_ref, [owner_ref[me + s] for s in range(slots)], theta_ref.shape[0], plan_ref
            )
        h, color, dz, fx, fy = e
        if (dz, fx, fy) == (0, 0, 0):
            finish(h, color)
        forward(*e)

    chips = zdim * ydim * 2

    def waiting(n, count, group, color):
        part = out_ref.at[pl.ds(0, n), pl.ds(0, count)]
        return pltpu.make_async_remote_copy(
            src_ref=part, dst_ref=part, send_sem=send.at[group], recv_sem=drecv.at[color],
            device_id=partner, device_id_type=pl.DeviceIdType.MESH,
        )

    for color, (_, count, _) in enumerate(COLORS):
        waiting(held * chips, count, 0, color).wait_recv()
    for group, numbers in sent.items():
        count = COLORS[group % colors][1] if group < LINKS * colors else out_ref.shape[1]
        if len(set(numbers)) == 1:
            waiting(numbers[0], count, group, 0).wait_send()
            continue
        for place, number in enumerate(numbers):
            if number:
                pl.when(z == place)(waiting(number, count, group, 0).wait_send)


ORDER = (
    (1, 0, 0, 0, 0), (1, 1, 0, 0, 0), (1, 2, 0, 0, 0), (0, 0, -1, 0, 0), (0, 2, 0, 0, 1),
    (0, 0, 1, 0, 0), (1, 0, 1, 0, 0), (0, 1, 1, 0, 0), (1, 0, -1, 0, 0), (1, 1, 1, 0, 0),
    (1, 1, -1, 0, 0), (0, 2, 0, 1, 0), (0, 1, -1, 0, 0), (0, 0, 0, 1, 0), (1, 2, 0, 1, 0),
    (1, 0, 2, 0, 0), (1, 1, 0, 0, 1), (0, 1, 2, 0, 0), (1, 1, 2, 0, 0), (1, 1, -2, 0, 0),
    (0, 2, -1, 0, 0), (0, 1, -2, 0, 0), (1, 0, 0, 0, 1), (1, 2, -1, 1, 0), (0, 2, 1, 0, 0),
    (1, 0, -2, 0, 0), (1, 1, 0, 1, 0), (0, 0, 2, 0, 0), (1, 2, 1, 1, 0), (0, 1, 1, 0, 1),
    (0, 0, 1, 1, 0), (1, 1, -3, 0, 0), (1, 0, 1, 0, 1), (0, 1, 3, 0, 0), (0, 0, -2, 0, 0),
    (1, 0, 3, 0, 0), (1, 2, 0, 0, 1), (0, 2, 0, 1, 1), (1, 0, 0, 1, 0), (1, 2, 1, 0, 0),
    (1, 2, 1, 0, 1), (1, 1, 1, 1, 0), (1, 0, -3, 0, 0), (1, 2, 0, 1, 1), (1, 2, 2, 1, 0),
    (0, 0, -3, 0, 0), (0, 2, -1, 0, 1), (0, 2, -1, 1, 1), (0, 0, 3, 0, 0), (0, 1, 2, 0, 1),
    (0, 1, -3, 0, 0), (0, 2, -2, 0, 0), (1, 2, -1, 0, 0), (1, 1, 3, 0, 0), (0, 1, -2, 0, 1),
    (1, 0, -3, 1, 0), (0, 1, 0, 0, 1), (1, 0, 2, 1, 0), (0, 2, 1, 0, 1), (1, 1, 1, 0, 1),
    (1, 0, -1, 1, 0), (0, 1, -3, 0, 1), (0, 0, -1, 1, 0), (0, 2, 1, 1, 1), (0, 2, 1, 1, 0),
    (0, 0, 1, 0, 1), (1, 1, -1, 0, 1), (1, 0, 3, 1, 0), (1, 2, 1, 1, 1), (0, 2, -1, 1, 0),
    (0, 1, 1, 1, 0), (0, 2, 2, 0, 0), (1, 2, 2, 0, 1), (0, 0, 3, 0, 1), (0, 0, -3, 1, 0),
    (1, 2, 2, 0, 0), (1, 1, 2, 0, 1), (0, 0, 3, 1, 0), (1, 2, 3, 1, 0), (1, 2, -1, 0, 1),
    (1, 0, -1, 0, 1), (0, 2, -2, 0, 1), (0, 0, -2, 0, 1), (1, 1, -3, 0, 1), (1, 2, -1, 1, 1),
    (1, 0, 1, 1, 0), (1, 1, -2, 0, 1), (0, 0, 2, 1, 0), (1, 0, 3, 0, 1), (0, 2, -3, 0, 0),
    (0, 0, -3, 0, 1), (0, 2, 2, 1, 1), (0, 0, -1, 0, 1), (1, 1, 3, 0, 1), (0, 1, -1, 0, 1),
    (0, 2, -2, 1, 0), (0, 1, 2, 1, 0), (1, 0, -2, 1, 0), (1, 2, -2, 0, 1), (0, 2, 2, 0, 1),
    (1, 2, 2, 1, 1), (0, 0, -2, 1, 0), (1, 1, 3, 1, 0), (1, 2, -2, 1, 0), (1, 0, -3, 1, 1),
    (0, 1, 3, 0, 1), (1, 0, 0, 1, 1), (0, 2, -3, 1, 0), (1, 2, -2, 0, 0), (0, 2, -3, 0, 1),
    (1, 2, -3, 1, 0), (1, 2, -3, 1, 1), (1, 1, 3, 1, 1), (1, 2, -2, 1, 1), (1, 0, 2, 1, 1),
    (0, 1, 2, 1, 1), (0, 0, 1, 1, 1), (0, 2, 2, 1, 0), (0, 1, 0, 1, 1), (1, 1, 1, 1, 1),
    (1, 1, 2, 1, 1), (1, 0, -2, 0, 1), (0, 1, 3, 1, 0), (0, 0, 0, 0, 1), (1, 1, -3, 1, 0),
    (1, 1, 2, 1, 0), (1, 0, -3, 0, 1), (1, 1, -1, 1, 1), (0, 1, -2, 1, 1), (0, 2, 3, 0, 1),
    (1, 1, -2, 1, 0), (1, 1, 0, 1, 1), (1, 2, 3, 0, 1), (0, 2, 3, 0, 0), (0, 0, 2, 0, 1),
    (0, 1, 3, 1, 1), (0, 1, -1, 1, 0), (1, 2, -3, 0, 1), (1, 1, -3, 1, 1), (0, 0, -3, 1, 1),
    (0, 1, -3, 1, 1), (0, 2, -3, 1, 1), (1, 1, -1, 1, 0), (0, 1, 1, 1, 1), (0, 2, -2, 1, 1),
    (0, 0, 0, 1, 1), (1, 0, -1, 1, 1), (1, 0, 3, 1, 1), (0, 0, -1, 1, 1), (0, 0, 3, 1, 1),
    (1, 2, 3, 1, 1), (0, 2, 3, 1, 1), (1, 1, -2, 1, 1), (1, 0, 2, 0, 1), (0, 1, -3, 1, 0),
    (1, 2, 3, 0, 0), (0, 0, -2, 1, 1), (1, 0, 1, 1, 1), (0, 1, 0, 1, 0), (0, 0, 2, 1, 1),
    (0, 1, -2, 1, 0), (1, 2, -3, 0, 0), (1, 0, -2, 1, 1), (0, 2, 3, 1, 0), (0, 1, -1, 1, 1),
)
PLAN_AT = 0


def exchange(effects, nominal, observed, variance, theta, nuisance_index, counts, tile_owner):
    nbins, nchan = lax.axis_size("bins"), lax.axis_size("chan")
    chans, size, channel_width = effects.shape
    rows, width = 2 * GW + EXTRA, GW
    held = chans // nbins
    hbm = pl.BlockSpec(memory_space=pltpu.HBM)
    vmem = pl.BlockSpec(memory_space=pltpu.VMEM)
    chips = nchan * nbins // 2
    slots = tile_owner.shape[0] // (nchan * nbins)
    colors = len(COLORS)
    operands = (
        nuisance_index, counts, effects, nominal, observed, variance,
        theta.reshape(-1, 1, GW), tile_owner,
    )
    return pl.pallas_call(
        functools.partial(exchange_kernel, 2, slots),
        in_specs=[hbm] * len(operands),
        out_specs=[vmem, vmem],
        out_shape=[
            jax.ShapeDtypeStruct((nchan * chans, rows, width), jnp.float32),
            jax.ShapeDtypeStruct((8, 4 * nchan * chans), jnp.int32),
        ],
        scratch_shapes=[
            pltpu.VMEM((chans, size, channel_width), jnp.bfloat16),
            pltpu.VMEM((chans, rows, width), jnp.float32),
            pltpu.VMEM((2 * held, rows, width), jnp.float32),
            pltpu.VMEM((held, rows, width), jnp.float32),
            pltpu.VMEM((held, rows, width), jnp.float32),
            pltpu.VMEM((2, channel_width + 16, size), jnp.bfloat16),
            pltpu.VMEM(nominal.shape, nominal.dtype),
            pltpu.VMEM(observed.shape, observed.dtype),
            pltpu.VMEM(variance.shape, variance.dtype),
            pltpu.VMEM((theta.shape[0] // GW, 1, GW), theta.dtype),
            pltpu.VMEM(nuisance_index.shape, jnp.int32),
            pltpu.SMEM((chans, nuisance_index.shape[1]), jnp.int32),
            pltpu.SMEM(counts.shape, jnp.int32),
            pltpu.SMEM(tile_owner.shape, jnp.int32),
            pltpu.SemaphoreType.DMA((chans,)),
            pltpu.SemaphoreType.DMA((8,)),
            pltpu.SemaphoreType.DMA((2 * held,)),
            pltpu.SemaphoreType.DMA((held, colors)),
            pltpu.SemaphoreType.DMA((held, colors, chips)),
            pltpu.SemaphoreType.DMA((colors,)),
            pltpu.SemaphoreType.DMA((LINKS * colors + 1,)),
        ],
        compiler_params=pltpu.CompilerParams(
            collective_id=0, has_side_effects=True, vmem_limit_bytes=32 * 2**20
        ),
        name="exchange",
    )(*[pltpu.with_memory_space_constraint(a, pltpu.HBM) for a in operands])


def fill_kernel(
    plan_hbm, payload_ref, index_ref, theta_ref, tiles_ref, grad_hbm,
    plan_ref, grad_ref, held_tiles, sems, small_sems,
):
    slots = held_tiles.shape[0]
    per_tile = TILE // GW
    shift = per_tile.bit_length() - 1
    row = lax.broadcasted_iota(jnp.int32, (GW, GW), 0)
    col = lax.broadcasted_iota(jnp.int32, (GW, GW), 1)
    eye = (row == col).astype(jnp.float32)
    ahead = min(2, slots)

    get_plan = pltpu.make_async_copy(plan_hbm, plan_ref, small_sems.at[0])
    put_grad = pltpu.make_async_copy(grad_ref, grad_hbm, small_sems.at[1])
    get_plan.start()

    def put(s):
        return pltpu.make_async_copy(held_tiles.at[s], tiles_ref.at[s], sems.at[s])

    def clear(s):
        held_tiles[s] = jnp.zeros((TILE, TILE), jnp.float32)

    for s in range(ahead):
        clear(s)

    mine = grad_ref.shape[0]
    device = lax.axis_index("chan") * lax.axis_size("bins") + lax.axis_index("bins")
    total_groups = theta_ref.shape[0]
    first = device * total_groups // (lax.axis_size("chan") * lax.axis_size("bins"))
    gshift = GW.bit_length() - 1
    for m in range(mine):
        acc = theta_ref[first + m]
        for r in range(2):
            hit = (index_ref[:, r * GW : (r + 1) * GW] >> gshift) == first + m
            acc += jnp.sum(jnp.where(hit, payload_ref[:, 2 * GW + r], 0.0), axis=0, keepdims=True)
        grad_ref[m] = acc
    put_grad.start()
    get_plan.wait()

    def one_tile(s, _):
        @pl.when(plan_ref[2, s] == 1)
        def _():
            for r in range(per_tile):
                held_tiles[s, r * GW : (r + 1) * GW, r * GW : (r + 1) * GW] = eye

        start, end = plan_ref[1, s], plan_ref[1, s + 1]

        def block_of(i):
            valid = i < end
            code = plan_ref[0, jnp.minimum(i, end - 1)]
            kind = code & 3
            rc = (code >> 2) & (per_tile - 1)
            rr = (code >> (2 + shift)) & (per_tile - 1)
            c = code >> (2 + 2 * shift)
            block = payload_ref[c, pl.ds(pl.multiple_of((kind >> 1) * GW, GW), GW)]
            side = jnp.where(kind == 0, row - col, jnp.where(kind == 1, col - row, kind - 2))
            value = jnp.where(side > 0, block.T, block)
            diag = payload_ref[c, 2 * GW + 2 : 2 * GW + 3]
            value = jnp.where(jnp.logical_and(kind == 1, row == col), diag, value)
            at = (
                s,
                pl.ds(pl.multiple_of(rr * GW, GW), GW),
                pl.ds(pl.multiple_of(rc * GW, GW), GW),
            )
            return at, jnp.where(valid, value, 0.0)

        def accumulate(i, _):
            for at, value in [block_of(start + i * TOGETHER + j) for j in range(TOGETHER)]:
                held_tiles[at] += value
            return 0

        lax.fori_loop(0, (end - start + TOGETHER - 1) // TOGETHER, accumulate, 0)
        put(s).start()

        @pl.when(s + ahead < slots)
        def _():
            clear(s + ahead)

        return 0

    lax.fori_loop(0, slots, one_tile, 0)

    def drain(s, _):
        put(s).wait()
        return 0

    lax.fori_loop(0, slots, drain, 0)
    put_grad.wait()


def fill(payload, plan, theta, nuisance_index, slots, mine):
    chans, rows = payload.shape[:2]
    vmem = pl.BlockSpec(memory_space=pltpu.VMEM)
    hbm = pl.BlockSpec(memory_space=pltpu.HBM)
    return pl.pallas_call(
        fill_kernel,
        in_specs=[vmem, vmem, vmem, vmem],
        out_specs=[hbm, hbm],
        out_shape=[
            jax.ShapeDtypeStruct((slots, TILE, TILE), jnp.float32),
            jax.ShapeDtypeStruct((mine, 1, GW), jnp.float32),
        ],
        scratch_shapes=[
            pltpu.SMEM(plan.shape, plan.dtype),
            pltpu.VMEM((mine, 1, GW), jnp.float32),
            pltpu.VMEM((slots, TILE, TILE), jnp.float32),
            pltpu.SemaphoreType.DMA((slots,)),
            pltpu.SemaphoreType.DMA((2,)),
        ],
        compiler_params=pltpu.CompilerParams(
            vmem_limit_bytes=4 * chans * (rows + EXTRA) * GW + 4 * slots * TILE * TILE + 4 * 2**20
        ),
        name="fill",
    )(plan, payload, nuisance_index, theta.reshape(-1, 1, GW))


def local(effects, nominal, observed, mc_variance, theta, nuisance_index, bin_counts, tile_owner):
    devices = lax.axis_size("chan") * lax.axis_size("bins")
    device = lax.axis_index("chan") * lax.axis_size("bins") + lax.axis_index("bins")
    total_nu = theta.shape[0]
    slice_len = total_nu // devices
    slots, mine = tile_owner.shape[0] // devices, max(1, slice_len // GW)
    chan_size, bins_size = lax.axis_size("chan"), lax.axis_size("bins")
    if bins_size == 4 and chan_size % 2 == 0 and chan_size // 2 <= DEEP and effects.shape[0] == 2 * bins_size and slice_len >= GW:
        payload, plan = exchange(
            effects, nominal, observed, mc_variance, theta, nuisance_index, bin_counts, tile_owner
        )
        tiles, grad = fill(payload, plan, theta, nuisance_index, slots, mine)
    else:
        groups = nuisance_index[:, ::GW] // GW
        arrays = (effects, nominal, observed, mc_variance, theta, groups, bin_counts)
        summed = lax.psum_scatter(curvature(*arrays), "bins", scatter_dimension=0, tiled=True)
        payload = lax.all_gather(summed, ("chan", "bins"), axis=0, tiled=True)
        tiles, grad = place(payload, theta, groups, tile_owner, slots, mine)
    gradient = grad.reshape(-1)
    if slice_len < GW:
        gradient = lax.dynamic_slice_in_dim(gradient, device * slice_len % GW, slice_len, 0)
    return (tiles, gradient)


def solution(mesh):
    return jax.shard_map(
        local,
        mesh=mesh,
        in_specs=(
            P("chan", "bins", None),
            P("chan", "bins"),
            P("chan", "bins"),
            P("chan", "bins"),
            P(),
            P(),
            P("chan"),
            P(),
        ),
        out_specs=(P(("chan", "bins"), None, None), P(("chan", "bins"))),
        check_vma=False,
    )
```
